256 devices in a mesh: models: 2 (over y), leaf: 128 (over x, z, core).
Axes of the slice: x: 4, y: 2, z: 16, core: 2. Of those that a mesh axis runs over, the one named last changes fastest.
The devices are a block of a 4x16x16 slice.
Arguments:
- slip_rate: float32 [1048576], P(('models', 'leaf')), parts along dimension 0, may hold values from -6 to 6
- near_blocks: bfloat16 [4096, 3, 256, 256], P(('models', 'leaf')), parts along dimension 0, may hold values from -0.21875 to 0.21875
- near_index: int32 [4096, 3], P(('models', 'leaf')), parts along dimension 0, may hold values from 0 to 2047, as said below
- far_left: bfloat16 [11, 32, 1048576], P(None, None, ('models', 'leaf')), parts along dimension 2, may hold values from -1 to 1
- far_right: bfloat16 [11, 32, 1048576], P(None, None, ('models', 'leaf')), parts along dimension 2, may hold values from -6 to 6
- far_ranks: int32 [4096, 11], P(('models', 'leaf')), parts along dimension 0, may hold values from 8 to 32
Outputs:
- first_stress: float32 [1048576], P(('models', 'leaf')), parts along dimension 0
- second_stress: float32 [1048576], P(('models', 'leaf')), parts along dimension 0
The draws below stay inside these ranges and needn't reach their ends.
There are 2 independent parts, one for each index of `models`. The reference program is written for one: setup_inputs(seed, part) draws one part's arguments, and reference() takes and returns one part's arrays. A program takes and returns all parts, laid end to end along the dimension named above; each array names one. Nothing has to cross between parts.
Inputs may be any that keep to these rules, and one draw needn't show every extreme that they name: near_index[i, 0] = i; every other entry is a leaf j != i with |j - i| <= 16, and distance 16 occurs.
All inputs are finite; a program needn't handle non-finite values.
Results may differ from the reference program's by a relative error of at most 0.0045.
Values may be sent and summed in bfloat16 or wider, within the bound.
A program may use at most 64 MiB of HBM per device.

```python
import math
import jax
import jax.numpy as jnp
from jax import lax

LEAF = 256
RANK = 32
NEAR = 3
LEAVES_DEV = 16
LEAVES = 2048
PATCHES = 524288
LEVELS = 11


def draw_near_index(key, part):
    base_key = jax.random.fold_in(key, 11)
    key_size, key_sign = jax.random.split(base_key)
    distance = jax.random.randint(key_size, (LEAVES, NEAR - 1), 1, LEAVES_DEV + 1)
    direction = jax.random.randint(key_sign, (LEAVES, NEAR - 1), 0, 2) * 2 - 1
    anchor = jnp.arange(LEAVES, dtype=jnp.int32)[:, None]
    target = anchor + direction * distance
    target = jnp.where((target < 0) | (target >= LEAVES), anchor - direction * distance, target)
    return jnp.concatenate([anchor, target], axis=1).astype(jnp.int32)


def set_ends(array, rng, smallest, high):
    longest = array.shape.index(max(array.shape))
    spots = []
    for shift in (0, 1):
        where = [jax.random.randint(jax.random.fold_in(rng, axis), (), 0, length) for axis, length in enumerate(array.shape)]
        where[longest] = (where[longest] + shift) % array.shape[longest]
        spots.append(tuple(where))
    return array.at[spots[0]].set(smallest).at[spots[1]].set(high)


def block_scale(rng, extent, cuts, low, high):
    def one(position, shards_of):
        steps = jax.random.uniform(jax.random.fold_in(jax.random.fold_in(rng, 6), position), (shards_of,), jnp.float32, low / len(cuts), high / len(cuts))
        return jnp.repeat(jnp.exp(steps), extent[position] // shards_of).reshape((-1,) + (1,) * (len(extent) - position - 1))

    level = one(*cuts[0])
    for cut in cuts[1:]:
        level = level * one(*cut)
    return level


def scatter_about(stream_key, dims, spread, limit, shards=(), kind=jnp.bfloat16):
    values = jax.random.normal(stream_key, dims, jnp.float32) * spread
    if len(shards) > 0:
        values = block_scale(stream_key, dims, shards, -0.22, 0.18) * values
    return jnp.clip(values, min=-limit, max=limit).astype(kind)


def setup_inputs(seed: int = 0, part: int = 0) -> dict:
    splits = jax.random.split(jax.random.key(seed), 7)
    own_keys = jax.random.split(jax.random.fold_in(splits[6], part), 7)
    return {
        "slip_rate": scatter_about(own_keys[0], (PATCHES,), 1.0, 6.0, ((0, 128),), jnp.float32),
        "near_blocks": scatter_about(own_keys[1], (LEAVES, NEAR, LEAF, LEAF), (NEAR * LEAF) ** -0.5, 0.21875, ((0, 128),)),
        "near_index": draw_near_index(jax.random.fold_in(jax.random.fold_in(splits[6], part), 71), part),
        "far_left": scatter_about(own_keys[3], (LEVELS, RANK, PATCHES), RANK ** -0.5, 1.0, ((2, 128),)),
        "far_right": scatter_about(own_keys[4], (LEVELS, RANK, PATCHES), 1.0, 6.0, ((2, 128),)),
        "far_ranks": set_ends(jax.random.randint(own_keys[5], (LEAVES, LEVELS), RANK // 4, RANK + 1), jax.random.fold_in(own_keys[5], 1), RANK // 4, RANK).astype(jnp.int32),
    }


def matvec(operand, near_blocks, near_index, far_left, far_right, far_ranks):
    leaves = near_blocks.shape[0]
    leaf_size = near_blocks.shape[2]
    levels = far_left.shape[0]
    rank_cols = far_left.shape[1]
    slip_rows = operand.reshape(leaves, leaf_size)
    picked = slip_rows[near_index].astype(jnp.float32)
    result = jnp.einsum('ikpq,ikq->ip', near_blocks.astype(jnp.float32), picked)
    rank_iota = jnp.arange(rank_cols, dtype=jnp.int32)
    rows_float = slip_rows.astype(jnp.float32)
    for level_no in range(levels):
        span_size = 2 ** level_no
        right_part = far_right[level_no].reshape(rank_cols, leaves, leaf_size).astype(jnp.float32)
        projected = jnp.einsum('rcp,cp->cr', right_part, rows_float)
        cluster_sums = projected.reshape(leaves // span_size, span_size, rank_cols).sum(axis=1)
        cluster_sums = cluster_sums * (1.0 / math.sqrt(leaf_size * span_size))
        partner = cluster_sums.reshape(-1, 2, rank_cols)[:, ::-1, :].reshape(-1, rank_cols)
        partner = jnp.repeat(partner, span_size, axis=0)
        masked = jnp.where(rank_iota[None, :] < far_ranks[:, level_no:level_no + 1], partner, 0.0)
        weights = lax.optimization_barrier(masked.astype(jnp.bfloat16))
        left_part = far_left[level_no].reshape(rank_cols, leaves, leaf_size).astype(jnp.float32)
        result = result + jnp.einsum('rcp,cr->cp', left_part, weights.astype(jnp.float32))
    return result.reshape(-1)

def reference(slip_rate, near_blocks, near_index, far_left, far_right, far_ranks):
    slip_bf = lax.optimization_barrier(slip_rate.astype(jnp.bfloat16))
    first_stress = matvec(slip_bf, near_blocks, near_index, far_left, far_right, far_ranks)
    relaxed = slip_rate + jnp.tanh(first_stress / 3.0)
    relaxed_bf = lax.optimization_barrier(relaxed.astype(jnp.bfloat16))
    second_stress = matvec(relaxed_bf, near_blocks, near_index, far_left, far_right, far_ranks)
    return (first_stress, second_stress)
```

```python
import functools
import math

import jax
import jax.numpy as jnp
from jax import lax
from jax.experimental import pallas as pl
from jax.experimental.pallas import tpu as pltpu
from jax.sharding import PartitionSpec as P

MESH = pl.DeviceIdType.MESH
F32 = jnp.float32
BF16 = jnp.bfloat16
LANES = 128
FAR_BITS = 2
NT = (((1,), (1,)), ((), ()))
NN = (((1,), (0,)), ((), ()))


def dot(a, b, dims):
    return lax.dot_general(a, b, dims, preferred_element_type=F32)


def kernel(
    shape,
    slip_hbm, ranks_hbm, index_hbm, right_hbm, near_hbm, left_hbm,
    first_hbm, second_hbm,
    slip, ranks, index, right, near, left, out, own, halo, masks,
    sums, got, plane_sums, got_far,
    load_sem, out_sem, halo_send, halo_recv, sums_send, sums_recv, far_send, far_recv,
):
    count, leaves, nears, leaf, levels, rank = shape
    local_levels = leaves.bit_length() - 1
    cross = levels - local_levels
    plane_bits = cross - FAR_BITS
    plane = 2**plane_bits
    groups = 2**FAR_BITS
    me = lax.axis_index("leaf")

    def peer_of(delta):
        return jnp.bitwise_xor(me, delta)

    right_of = lax.rem(me + 1, count)
    left_of = lax.rem(me + count - 1, count)

    barrier = pltpu.get_barrier_semaphore()
    peers = [right_of, left_of]
    peers += [peer_of(t) for t in range(1, plane)]
    peers += [peer_of(plane * g) for g in range(1, groups)]
    for peer in peers:
        pl.semaphore_signal(barrier, inc=1, device_id={"leaf": peer}, device_id_type=MESH)

    high = local_levels - 1
    loads = [
        pltpu.make_async_copy(slip_hbm, slip, load_sem.at[0]),
        pltpu.make_async_copy(right_hbm.at[pl.ds(high, levels - high)],
                              right.at[pl.ds(high, levels - high)], load_sem.at[1]),
        pltpu.make_async_copy(ranks_hbm, ranks, load_sem.at[2]),
        pltpu.make_async_copy(index_hbm, index, load_sem.at[3]),
        pltpu.make_async_copy(right_hbm.at[pl.ds(0, high)], right.at[pl.ds(0, high)], load_sem.at[4]),
        pltpu.make_async_copy(near_hbm, near, load_sem.at[5]),
        pltpu.make_async_copy(left_hbm, left, load_sem.at[6]),
    ]
    for load in loads:
        load.start()

    row = lax.broadcasted_iota(jnp.int32, (leaves, leaf), 0)
    row_l = lax.broadcasted_iota(jnp.int32, (leaves, LANES), 0)
    lane = lax.broadcasted_iota(jnp.int32, (leaves, LANES), 1)
    lane1 = lax.broadcasted_iota(jnp.int32, (1, LANES), 1)

    def project(vf, start, stop):
        rows = (stop - start) * rank
        total = jnp.zeros((leaves, rows), F32)
        for c in range(leaves):
            lhs = jnp.where(row == c, vf, 0.0).astype(BF16)
            rhs = right[start:stop, :, c * leaf:(c + 1) * leaf].reshape(rows, leaf)
            total += dot(lhs, rhs, NT)
        return total

    def apply_far(total, weights, start, stop):
        rows = (stop - start) * rank
        row_w = lax.broadcasted_iota(jnp.int32, weights.shape, 0)
        for i in range(leaves):
            lhs = jnp.where(row_w == i, weights, 0.0).astype(BF16)[:, :rows]
            rhs = left[start:stop, :, i * leaf:(i + 1) * leaf].reshape(rows, leaf)
            total += dot(lhs, rhs, NN)
        return total

    def scale_of(level):
        return 1.0 / math.sqrt(leaf * 2**level)

    def product(step, vf):
        own[step] = vf.astype(BF16)
        if step == 0:
            loads[1].wait()
        summed = project(vf, high, levels)
        device_sums = jnp.sum(summed, axis=0, keepdims=True)
        parts = [device_sums[:, :LANES], device_sums[:, LANES:]]
        for b in range(plane_bits):
            place = (b + 1) * rank
            shift = (rank - place) % LANES
            source = parts[place // LANES]
            moved = pltpu.roll(source, shift, 1) if shift else source
            sums[step, b] = jnp.where(lane1 < 2 * rank, moved, parts[1])
        if step == 0:
            pl.semaphore_wait(barrier, len(peers))
        for t in range(1, plane):
            pltpu.make_async_remote_copy(
                src_ref=sums.at[step, t.bit_length() - 1],
                dst_ref=got.at[step, t],
                send_sem=sums_send.at[step],
                recv_sem=sums_recv.at[step],
                device_id={"leaf": peer_of(t)},
                device_id_type=MESH,
            ).start()
        halos = []
        for side, peer in ((0, right_of), (1, left_of)):
            copy = pltpu.make_async_remote_copy(
                src_ref=own.at[step],
                dst_ref=halo.at[step, side],
                send_sem=halo_send.at[step, side],
                recv_sem=halo_recv.at[step, side],
                device_id={"leaf": peer},
                device_id_type=MESH,
            )
            copy.start()
            halos.append(copy)

        if step == 0:
            loads[2].wait()
            loads[3].wait()
            for group in range(-(-levels * rank // LANES)):
                limit = jnp.zeros((leaves, LANES), jnp.int32)
                for part in range(LANES // rank):
                    level = group * (LANES // rank) + part
                    if level < levels:
                        held = jnp.broadcast_to(ranks[:, level:level + 1], (leaves, LANES))
                        limit = jnp.where(lane // rank == part, held, limit)
                masks[group] = (lane % rank < limit).astype(F32)
            loads[4].wait()

        below = project(vf, 0, high)
        chosen = jnp.zeros((leaves, LANES), F32)
        fine = jnp.concatenate([below, summed[:, :rank]], axis=1)
        cluster_r = lax.broadcasted_iota(jnp.int32, (leaves, leaves), 0)
        cluster_c = lax.broadcasted_iota(jnp.int32, (leaves, leaves), 1)
        for level in range(local_levels):
            pick = (cluster_c >> level) == ((cluster_r >> level) ^ 1)
            partner = lax.dot_general(
                pick.astype(F32), fine, NN,
                precision=lax.Precision.HIGHEST, preferred_element_type=F32,
            )
            chosen = jnp.where(lane // rank == level, partner * scale_of(level), chosen)
        if step == 0:
            loads[6].wait()
        total = apply_far(
            jnp.zeros((leaves, leaf), F32), jnp.where(masks[0] > 0.0, chosen, 0.0), 0, local_levels
        )

        for copy in halos:
            copy.wait_recv()
        if step == 0:
            loads[5].wait()
        extended = jnp.concatenate([halo[step, 0], own[step], halo[step, 1]], axis=0)
        first_leaf = (me - 1) * leaves
        spot = lax.broadcasted_iota(jnp.int32, (leaves, 3 * leaves), 1) + first_leaf
        for k in range(nears):
            hot = (jnp.broadcast_to(index[:, k:k + 1], (leaves, 3 * leaves)) == spot)
            picked = dot(hot.astype(F32).astype(BF16), extended, NN)
            for i in range(leaves):
                lhs = jnp.where(row == i, picked, 0.0).astype(BF16)
                total += dot(lhs, near[i, k], NT)

        pltpu.make_async_copy(
            got.at[step, pl.ds(1, plane - 1)], got.at[step, pl.ds(1, plane - 1)], sums_recv.at[step]
        ).wait()
        by_level = []
        for b in range(plane_bits):
            terms = [got[step, t] for t in range(2**b, 2 ** (b + 1))]
            while len(terms) > 1:
                terms = [x + y for x, y in zip(terms[::2], terms[1::2])]
            by_level.append(terms[0])
        everything = parts[1]
        for term in by_level:
            everything = everything + term
        plane_sums[step] = everything
        for g in range(1, groups):
            pltpu.make_async_remote_copy(
                src_ref=plane_sums.at[step],
                dst_ref=got_far.at[step, g],
                send_sem=far_send.at[step],
                recv_sem=far_recv.at[step],
                device_id={"leaf": peer_of(plane * g)},
                device_id_type=MESH,
            ).start()
        per = LANES // rank
        columns = []
        for group in range(-(-plane_bits // per)):
            held = jnp.zeros((1, LANES), F32)
            for part in range(per):
                b = group * per + part
                if b < plane_bits:
                    shift = (part - 1) * rank % LANES
                    value = by_level[b] * scale_of(local_levels + b)
                    value = pltpu.roll(value, shift, 1) if shift else value
                    held = jnp.where(lane1 // rank == part, value, held)
            columns.append(
                jnp.where(masks[group + 1] > 0.0, jnp.broadcast_to(held, (leaves, LANES)), 0.0)
            )
        total = apply_far(
            total, jnp.concatenate(columns, axis=1), local_levels, local_levels + plane_bits
        )

        pltpu.make_async_copy(
            got_far.at[step, pl.ds(1, groups - 1)], got_far.at[step, pl.ds(1, groups - 1)],
            far_recv.at[step],
        ).wait()
        near_far = got_far[step, 1] * scale_of(levels - 2)
        far_far = (got_far[step, 2] + got_far[step, 3]) * scale_of(levels - 1)
        held = jnp.where(lane1 < 3 * rank, near_far, far_far)
        held = pltpu.roll(held, 2 * rank, 1)
        shift = (plane_bits + local_levels) * rank % LANES
        mask = pltpu.roll(masks[(plane_bits + local_levels) * rank // LANES], (LANES - shift) % LANES, 1)
        last = jnp.where(mask > 0.0, jnp.broadcast_to(held, (leaves, LANES)), 0.0)
        total = apply_far(total, last, levels - FAR_BITS, levels)
        out[step, pl.ds(0, leaves, 2), :] = total[:, :LANES]
        out[step, pl.ds(1, leaves, 2), :] = total[:, LANES:]
        return total

    loads[0].wait()
    slip_rate = jnp.concatenate([slip[pl.ds(0, leaves, 2), :], slip[pl.ds(1, leaves, 2), :]], axis=1)
    first = product(0, slip_rate.astype(BF16).astype(F32))
    first_out = pltpu.make_async_copy(out.at[0], first_hbm, out_sem.at[0])
    first_out.start()
    relaxed = slip_rate + jnp.tanh(first / 3.0)
    product(1, relaxed.astype(BF16).astype(F32))
    second_out = pltpu.make_async_copy(out.at[1], second_hbm, out_sem.at[1])
    second_out.start()

    for step in range(2):
        for side in range(2):
            pltpu.make_async_copy(own.at[step], own.at[step], halo_send.at[step, side]).wait()
        pltpu.make_async_copy(
            got.at[step, pl.ds(1, plane - 1)], got.at[step, pl.ds(1, plane - 1)], sums_send.at[step]
        ).wait()
        pltpu.make_async_copy(
            got_far.at[step, pl.ds(1, groups - 1)], got_far.at[step, pl.ds(1, groups - 1)],
            far_send.at[step],
        ).wait()
    first_out.wait()
    second_out.wait()


def local(count, slip_rate, near_blocks, near_index, far_left, far_right, far_ranks):
    leaves, nears, leaf, _ = near_blocks.shape
    levels, rank, patches = far_left.shape
    cross = levels - (leaves.bit_length() - 1)
    plane_bits = cross - FAR_BITS
    plane, groups = 2**plane_bits, 2**FAR_BITS
    assert leaf == 2 * LANES and 4 * rank == LANES and 2**cross == count
    flat = (patches // LANES, LANES)
    anywhere = pl.BlockSpec(memory_space=pl.ANY)
    first, second = pl.pallas_call(
        functools.partial(kernel, (count, leaves, nears, leaf, levels, rank)),
        out_shape=[jax.ShapeDtypeStruct(flat, F32)] * 2,
        in_specs=[anywhere] * 6,
        out_specs=[anywhere] * 2,
        scratch_shapes=[
            pltpu.VMEM(flat, F32),
            pltpu.VMEM(far_ranks.shape, jnp.int32),
            pltpu.VMEM(near_index.shape, jnp.int32),
            pltpu.VMEM(far_right.shape, BF16),
            pltpu.VMEM(near_blocks.shape, BF16),
            pltpu.VMEM(far_left.shape, BF16),
            pltpu.VMEM((2,) + flat, F32),
            pltpu.VMEM((2, leaves, leaf), BF16),
            pltpu.VMEM((2, 2, leaves, leaf), BF16),
            pltpu.VMEM((-(-levels * rank // LANES), leaves, LANES), F32),
            pltpu.VMEM((2, plane_bits, 1, LANES), F32),
            pltpu.VMEM((2, plane, 1, LANES), F32),
            pltpu.VMEM((2, 1, LANES), F32),
            pltpu.VMEM((2, groups, 1, LANES), F32),
            pltpu.SemaphoreType.DMA((7,)),
            pltpu.SemaphoreType.DMA((2,)),
            pltpu.SemaphoreType.DMA((2, 2)),
            pltpu.SemaphoreType.DMA((2, 2)),
            pltpu.SemaphoreType.DMA((2,)),
            pltpu.SemaphoreType.DMA((2,)),
            pltpu.SemaphoreType.DMA((2,)),
            pltpu.SemaphoreType.DMA((2,)),
        ],
        compiler_params=pltpu.CompilerParams(collective_id=0, has_side_effects=True),
        name="hmatrix",
    )(slip_rate.reshape(flat), far_ranks, near_index, far_right, near_blocks, far_left)
    return first.reshape(-1), second.reshape(-1)


def solution(mesh):
    both = ("models", "leaf")
    in_specs = (
        P(both), P(both, None, None, None), P(both, None),
        P(None, None, both), P(None, None, both), P(both, None),
    )
    return jax.shard_map(
        functools.partial(local, mesh.shape["leaf"]), mesh=mesh, in_specs=in_specs,
        out_specs=(P(both), P(both)), check_vma=False,
    )
```

```python
import functools
import math

import jax
import jax.numpy as jnp
from jax import lax
from jax.experimental import pallas as pl
from jax.experimental.pallas import tpu as pltpu
from jax.sharding import PartitionSpec as P

MESH = pl.DeviceIdType.MESH
F32 = jnp.float32
BF16 = jnp.bfloat16
LANES = 128
FAR_BITS = 2
NT = (((1,), (1,)), ((), ()))
NN = (((1,), (0,)), ((), ()))
TN = (((0,), (0,)), ((), ()))
PIECES = 4


def dot(a, b, dims):
    return lax.dot_general(a, b, dims, preferred_element_type=F32)


def kernel(
    shape,
    slip_hbm, ranks_hbm, index_hbm, right_hbm, near_hbm, left_hbm,
    out,
    slip, ranks, index, right, near, left, own, halo, masks,
    sums, got, plane_sums, got_far,
    load_sem, piece_sem, halo_send, halo_recv, sums_send, sums_recv, far_send, far_recv,
):
    count, leaves, nears, leaf, levels, rank = shape
    local_levels = leaves.bit_length() - 1
    cross = levels - local_levels
    plane_bits = cross - FAR_BITS
    plane = 2**plane_bits
    groups = 2**FAR_BITS
    me = lax.axis_index("leaf")

    def peer_of(delta):
        return jnp.bitwise_xor(me, delta)

    right_of = lax.rem(me + 1, count)
    left_of = lax.rem(me + count - 1, count)

    chips = plane // 2
    def reach(t):
        return max(min(abs(z - (z ^ t // 2)), chips - abs(z - (z ^ t // 2))) for z in range(chips))
    deltas = sorted(range(1, plane), key=reach, reverse=True)

    high = local_levels - 1
    piece = leaves // PIECES * leaf
    loads = [
        pltpu.make_async_copy(slip_hbm, slip, load_sem.at[0]),
        pltpu.make_async_copy(left_hbm, left, load_sem.at[1]),
        pltpu.make_async_copy(ranks_hbm, ranks, load_sem.at[2]),
        pltpu.make_async_copy(index_hbm, index, load_sem.at[3]),
        pltpu.make_async_copy(right_hbm.at[pl.ds(0, high)], right.at[pl.ds(0, high)], load_sem.at[4]),
        pltpu.make_async_copy(near_hbm, near, load_sem.at[5]),
    ]
    pieces = []
    for n in range(PIECES):
        part = (pl.ds(high, levels - high), slice(None), pl.ds(n * piece, piece))
        pieces.append(pltpu.make_async_copy(right_hbm.at[part], right.at[part], piece_sem.at[n]))
    loads[0].start()
    for load in pieces:
        load.start()

    barrier = pltpu.get_barrier_semaphore()
    peers = [peer_of(t) for t in deltas]
    peers += [peer_of(plane * g) for g in range(1, groups)]
    peers += [right_of, left_of]
    for peer in peers:
        pl.semaphore_signal(barrier, inc=1, device_id={"leaf": peer}, device_id_type=MESH)
    for load in (loads[2], loads[3], loads[4], loads[1], loads[5]):
        load.start()

    row = lax.broadcasted_iota(jnp.int32, (leaves, leaf), 0)
    row_l = lax.broadcasted_iota(jnp.int32, (leaves, LANES), 0)
    lane = lax.broadcasted_iota(jnp.int32, (leaves, LANES), 1)
    lane1 = lax.broadcasted_iota(jnp.int32, (1, LANES), 1)

    def project(vf, start, stop, ready=()):
        rows = (stop - start) * rank
        total = jnp.zeros((leaves, rows), F32)
        for c in range(leaves):
            if ready and c % (leaves // PIECES) == 0:
                ready[c // (leaves // PIECES)].wait()
            lhs = jnp.where(row == c, vf, 0.0).astype(BF16)
            rhs = right[start:stop, :, c * leaf:(c + 1) * leaf].reshape(rows, leaf)
            total += dot(lhs, rhs, NT)
        return total

    def apply_far(total, weights, start, stop):
        rows = (stop - start) * rank
        row_w = lax.broadcasted_iota(jnp.int32, weights.shape, 0)
        for i in range(leaves):
            lhs = jnp.where(row_w == i, weights, 0.0).astype(BF16)[:, :rows]
            rhs = left[start:stop, :, i * leaf:(i + 1) * leaf].reshape(rows, leaf)
            total += dot(lhs, rhs, NN)
        return total

    def scale_of(level):
        return 1.0 / math.sqrt(leaf * 2**level)

    def product(step, vf):
        own[step] = vf.astype(BF16)
        summed = project(vf, high, levels, () if step else pieces)
        device_sums = jnp.sum(summed, axis=0, keepdims=True)
        parts = [device_sums[:, :LANES], device_sums[:, LANES:]]
        for b in range(plane_bits):
            place = (b + 1) * rank
            shift = (rank - place) % LANES
            source = parts[place // LANES]
            moved = pltpu.roll(source, shift, 1) if shift else source
            sums[step, b] = jnp.where(lane1 < 2 * rank, moved, parts[1])
        if step == 0:
            pl.semaphore_wait(barrier, len(peers))
        for t in deltas:
            pltpu.make_async_remote_copy(
                src_ref=sums.at[step, t.bit_length() - 1],
                dst_ref=got.at[step, t],
                send_sem=sums_send.at[step],
                recv_sem=sums_recv.at[step],
                device_id={"leaf": peer_of(t)},
                device_id_type=MESH,
            ).start()
        halos = []
        for side, peer in ((0, right_of), (1, left_of)):
            copy = pltpu.make_async_remote_copy(
                src_ref=own.at[step],
                dst_ref=halo.at[step, side],
                send_sem=halo_send.at[step, side],
                recv_sem=halo_recv.at[step, side],
                device_id={"leaf": peer},
                device_id_type=MESH,
            )
            copy.start()
            halos.append(copy)

        if step == 0:
            loads[2].wait()
            loads[3].wait()
            for group in range(-(-levels * rank // LANES)):
                limit = jnp.zeros((leaves, LANES), jnp.int32)
                for part in range(LANES // rank):
                    level = group * (LANES // rank) + part
                    if level < levels:
                        held = jnp.broadcast_to(ranks[:, level:level + 1], (leaves, LANES))
                        limit = jnp.where(lane // rank == part, held, limit)
                masks[group] = (lane % rank < limit).astype(F32)
            loads[4].wait()

        below = project(vf, 0, high)
        chosen = jnp.zeros((leaves, LANES), F32)
        fine = jnp.concatenate([below, summed[:, :rank]], axis=1)
        cluster_r = lax.broadcasted_iota(jnp.int32, (leaves, leaves), 0)
        cluster_c = lax.broadcasted_iota(jnp.int32, (leaves, leaves), 1)
        for level in range(local_levels):
            pick = (cluster_c >> level) == ((cluster_r >> level) ^ 1)
            partner = lax.dot_general(
                pick.astype(F32), fine, NN,
                precision=lax.Precision.HIGHEST, preferred_element_type=F32,
            )
            chosen = jnp.where(lane // rank == level, partner * scale_of(level), chosen)
        if step == 0:
            loads[1].wait()
        total = apply_far(
            jnp.zeros((leaves, leaf), F32), jnp.where(masks[0] > 0.0, chosen, 0.0), 0, local_levels
        )

        for copy in halos:
            copy.wait_recv()
        if step == 0:
            loads[5].wait()
        extended = jnp.concatenate([halo[step, 0], own[step], halo[step, 1]], axis=0)
        first_leaf = (me - 1) * leaves
        spot = lax.broadcasted_iota(jnp.int32, (3 * leaves, leaves), 0) + first_leaf
        for k in range(nears):
            hot = jnp.broadcast_to(index[k:k + 1, :], (3 * leaves, leaves)) == spot
            picked = dot(hot.astype(F32).astype(BF16), extended, TN)
            for i in range(leaves):
                lhs = jnp.where(row == i, picked, 0.0).astype(BF16)
                total += dot(lhs, near[i, k], NT)

        pltpu.make_async_copy(
            got.at[step, pl.ds(1, plane - 1)], got.at[step, pl.ds(1, plane - 1)], sums_recv.at[step]
        ).wait()
        by_level = []
        for b in range(plane_bits):
            terms = [got[step, t] for t in range(2**b, 2 ** (b + 1))]
            while len(terms) > 1:
                terms = [x + y for x, y in zip(terms[::2], terms[1::2])]
            by_level.append(terms[0])
        everything = parts[1]
        for term in by_level:
            everything = everything + term
        plane_sums[step] = everything
        for g in range(1, groups):
            pltpu.make_async_remote_copy(
                src_ref=plane_sums.at[step],
                dst_ref=got_far.at[step, g],
                send_sem=far_send.at[step],
                recv_sem=far_recv.at[step],
                device_id={"leaf": peer_of(plane * g)},
                device_id_type=MESH,
            ).start()
        per = LANES // rank
        columns = []
        for group in range(-(-plane_bits // per)):
            held = jnp.zeros((1, LANES), F32)
            for part in range(per):
                b = group * per + part
                if b < plane_bits:
                    shift = (part - 1) * rank % LANES
                    value = by_level[b] * scale_of(local_levels + b)
                    value = pltpu.roll(value, shift, 1) if shift else value
                    held = jnp.where(lane1 // rank == part, value, held)
            columns.append(
                jnp.where(masks[group + 1] > 0.0, jnp.broadcast_to(held, (leaves, LANES)), 0.0)
            )
        total = apply_far(
            total, jnp.concatenate(columns, axis=1), local_levels, local_levels + plane_bits
        )

        pltpu.make_async_copy(
            got_far.at[step, pl.ds(1, groups - 1)], got_far.at[step, pl.ds(1, groups - 1)],
            far_recv.at[step],
        ).wait()
        near_far = got_far[step, 1] * scale_of(levels - 2)
        far_far = (got_far[step, 2] + got_far[step, 3]) * scale_of(levels - 1)
        held = jnp.where(lane1 < 3 * rank, near_far, far_far)
        held = pltpu.roll(held, 2 * rank, 1)
        shift = (plane_bits + local_levels) * rank % LANES
        mask = pltpu.roll(masks[(plane_bits + local_levels) * rank // LANES], (LANES - shift) % LANES, 1)
        last = jnp.where(mask > 0.0, jnp.broadcast_to(held, (leaves, LANES)), 0.0)
        total = apply_far(total, last, levels - FAR_BITS, levels)
        out[step, pl.ds(0, leaves, 2), :] = total[:, :LANES]
        out[step, pl.ds(1, leaves, 2), :] = total[:, LANES:]
        return total

    loads[0].wait()
    slip_rate = jnp.concatenate([slip[pl.ds(0, leaves, 2), :], slip[pl.ds(1, leaves, 2), :]], axis=1)
    first = product(0, slip_rate.astype(BF16).astype(F32))
    relaxed = slip_rate + jnp.tanh(first / 3.0)
    product(1, relaxed.astype(BF16).astype(F32))

    for step in range(2):
        for side in range(2):
            pltpu.make_async_copy(own.at[step], own.at[step], halo_send.at[step, side]).wait()
        pltpu.make_async_copy(
            got.at[step, pl.ds(1, plane - 1)], got.at[step, pl.ds(1, plane - 1)], sums_send.at[step]
        ).wait()
        pltpu.make_async_copy(
            got_far.at[step, pl.ds(1, groups - 1)], got_far.at[step, pl.ds(1, groups - 1)],
            far_send.at[step],
        ).wait()


def write(out, first, second, sem):
    copies = [pltpu.make_async_copy(out.at[n], ref, sem.at[n]) for n, ref in enumerate((first, second))]
    for copy in copies:
        copy.start()
    for copy in copies:
        copy.wait()


def local(count, slip_rate, near_blocks, near_index, far_left, far_right, far_ranks):
    leaves, nears, leaf, _ = near_blocks.shape
    levels, rank, patches = far_left.shape
    cross = levels - (leaves.bit_length() - 1)
    plane_bits = cross - FAR_BITS
    plane, groups = 2**plane_bits, 2**FAR_BITS
    assert leaf == 2 * LANES and 4 * rank == LANES and 2**cross == count
    flat = (patches // LANES, LANES)
    anywhere = pl.BlockSpec(memory_space=pl.ANY)
    out = pl.pallas_call(
        functools.partial(kernel, (count, leaves, nears, leaf, levels, rank)),
        out_shape=pltpu.VMEM((2,) + flat, F32),
        in_specs=[anywhere] * 6,
        out_specs=pl.BlockSpec(memory_space=pltpu.VMEM),
        scratch_shapes=[
            pltpu.VMEM(flat, F32),
            pltpu.VMEM(far_ranks.shape, jnp.int32),
            pltpu.VMEM(near_index.shape[::-1], jnp.int32),
            pltpu.VMEM(far_right.shape, BF16),
            pltpu.VMEM(near_blocks.shape, BF16),
            pltpu.VMEM(far_left.shape, BF16),
            pltpu.VMEM((2, leaves, leaf), BF16),
            pltpu.VMEM((2, 2, leaves, leaf), BF16),
            pltpu.VMEM((-(-levels * rank // LANES), leaves, LANES), F32),
            pltpu.VMEM((2, plane_bits, 1, LANES), F32),
            pltpu.VMEM((2, plane, 1, LANES), F32),
            pltpu.VMEM((2, 1, LANES), F32),
            pltpu.VMEM((2, groups, 1, LANES), F32),
            pltpu.SemaphoreType.DMA((6,)),
            pltpu.SemaphoreType.DMA((PIECES,)),
            pltpu.SemaphoreType.DMA((2, 2)),
            pltpu.SemaphoreType.DMA((2, 2)),
            pltpu.SemaphoreType.DMA((2,)),
            pltpu.SemaphoreType.DMA((2,)),
            pltpu.SemaphoreType.DMA((2,)),
            pltpu.SemaphoreType.DMA((2,)),
        ],
        compiler_params=pltpu.CompilerParams(collective_id=0, has_side_effects=True),
        name="hmatrix",
    )(slip_rate.reshape(flat), far_ranks, near_index.T, far_right, near_blocks, far_left)
    first, second = pl.pallas_call(
        write,
        out_shape=[jax.ShapeDtypeStruct(flat, F32)] * 2,
        in_specs=[pl.BlockSpec(memory_space=pltpu.VMEM)],
        out_specs=[anywhere] * 2,
        scratch_shapes=[pltpu.SemaphoreType.DMA((2,))],
        name="write",
    )(pltpu.with_memory_space_constraint(out, pltpu.VMEM))
    return first.reshape(-1), second.reshape(-1)


def solution(mesh):
    both = ("models", "leaf")
    in_specs = (
        P(both), P(both, None, None, None), P(both, None),
        P(None, None, both), P(None, None, both), P(both, None),
    )
    return jax.shard_map(
        functools.partial(local, mesh.shape["leaf"]), mesh=mesh, in_specs=in_specs,
        out_specs=(P(both), P(both)), check_vma=False,
    )
```

```python
import functools
import math

import jax
import jax.numpy as jnp
from jax import lax
from jax.experimental import pallas as pl
from jax.experimental.pallas import tpu as pltpu
from jax.sharding import PartitionSpec as P

MESH = pl.DeviceIdType.MESH
F32 = jnp.float32
BF16 = jnp.bfloat16
LANES = 128
FAR_BITS = 2
PIECES = 4
NEAR_UNROLL = 4
NT = (((1,), (1,)), ((), ()))
NN = (((1,), (0,)), ((), ()))
TN = (((0,), (0,)), ((), ()))


def dot(a, b, dims):
    return lax.dot_general(a, b, dims, preferred_element_type=F32)


def add_all(terms):
    terms = list(terms)
    while len(terms) > 1:
        odd = terms[len(terms) // 2 * 2:]
        terms = [x + y for x, y in zip(terms[::2], terms[1::2])] + odd
    return terms[0]


def kernel(
    shape,
    slip_hbm, ranks_hbm, index_hbm, right_hbm, near_hbm, left_hbm,
    out,
    slip, ranks, index, right, near, left, own, halo, masks, picks, sums,
    mail, got, known, relay, got_relay, plane_sums, got_plane, got_all, got_pair,
    load_sem, piece_sem, halo_send, halo_recv, level_send, level_recv, relay_send, relay_recv,
    plane_send, plane_recv, all_send, all_recv, pair_send, pair_recv, ready, near_ready,
):
    count, leaves, nears, leaf, levels, rank = shape
    local_levels = leaves.bit_length() - 1
    cross = levels - local_levels
    groups = 2**FAR_BITS
    plane = count // groups
    ring_bits = cross - FAR_BITS - 1
    ring = 2**ring_bits
    me = lax.axis_index("leaf")
    spot = lax.rem(me // 2, ring)

    def peer_of(far, step, core):
        return jnp.bitwise_xor(me, far * plane + step * 2 + core)

    def bit(j):
        return lax.rem(spot // 2**j, 2) == 1

    def target(peer):
        return dict(device_id={"leaf": peer}, device_id_type=MESH)

    right_of = lax.rem(me + 1, count)
    left_of = lax.rem(me + count - 1, count)
    far_first = [g for g in (2, 3, 1, 0) if g < groups]
    quad_bits = ring_bits - 2
    quad = 2 ** (quad_bits + 1)
    upper = range(quad_bits, ring_bits)
    relay_step = {quad_bits: ring // 4, quad_bits + 1: ring // 2 + ring // 4}
    half = ring // 2
    runs = [(ring_bits - 1, half, 1, half // 2), (ring_bits - 2, half - 1, -1, half // 2),
            (ring_bits - 1, half + half // 2, 1, half // 2)]
    runs += [(j, 2 ** (j + 1) - 1, -1, 2**j) for j in reversed(range(ring_bits - 2))]

    def run(first, stride, length, body):
        def trip(n, carry):
            body(first + stride * n)
            return carry

        lax.fori_loop(0, length, trip, 0)

    high = local_levels - 1
    piece = leaves // PIECES * leaf
    loads = [
        pltpu.make_async_copy(slip_hbm, slip, load_sem.at[0]),
        pltpu.make_async_copy(left_hbm, left, load_sem.at[1]),
        pltpu.make_async_copy(ranks_hbm, ranks, load_sem.at[2]),
        pltpu.make_async_copy(index_hbm, index, load_sem.at[3]),
        pltpu.make_async_copy(right_hbm.at[pl.ds(0, high)], right.at[pl.ds(0, high)], load_sem.at[4]),
        pltpu.make_async_copy(near_hbm, near, load_sem.at[5]),
    ]
    pieces = []
    for n in range(PIECES):
        part = (pl.ds(high, levels - high), slice(None), pl.ds(n * piece, piece))
        pieces.append(pltpu.make_async_copy(right_hbm.at[part], right.at[part], piece_sem.at[n]))
    loads[0].start()
    for load in pieces:
        load.start()

    barrier = pltpu.get_barrier_semaphore()

    def greet(peer):
        pl.semaphore_signal(barrier, inc=1, **target(peer))

    expected = quad - 1 + groups - 1
    for j, first_step, stride, length in runs:
        if j > quad_bits:
            @pl.when(jnp.logical_not(bit(j)))
            def _(first_step=first_step, stride=stride, length=length):
                def both(step):
                    for c in range(2):
                        greet(peer_of(0, step, c))
                run(first_step, stride, length, both)
    pl.when(bit(quad_bits))(lambda: greet(peer_of(0, relay_step[quad_bits], 0)))
    for t in reversed(range(1, quad)):
        greet(peer_of(0, t // 2, t % 2))
    for g in far_first[:-1]:
        greet(peer_of(g, 0, 0))
    top = jnp.logical_and(spot == ring - 1, lax.rem(me, 2) == 1)
    bottom = jnp.logical_and(spot == 0, lax.rem(me, 2) == 0)
    pl.when(jnp.logical_not(top))(lambda: greet(right_of))
    pl.when(bottom)(lambda: greet(left_of))
    expected = expected + jnp.where(bottom, 0, 1) + jnp.where(top, 1, 0)
    for j in upper:
        expected = expected + (
            jnp.where(bit(j), 2 ** (j + 1), 0) if j > quad_bits else jnp.where(bit(j), 0, 1)
        )
    for load in (loads[2], loads[3], loads[4], loads[1], loads[5]):
        load.start()

    row = lax.broadcasted_iota(jnp.int32, (leaves, leaf), 0)
    row_l = lax.broadcasted_iota(jnp.int32, (leaves, LANES), 0)
    lane = lax.broadcasted_iota(jnp.int32, (leaves, LANES), 1)
    lane1 = lax.broadcasted_iota(jnp.int32, (1, LANES), 1)

    def scale_of(level):
        return 1.0 / math.sqrt(leaf * 2**level)

    def by_lane(values):
        scale = jnp.zeros((1, LANES), F32)
        for part, value in enumerate(values):
            scale = jnp.where(lane1 // rank == part, value, scale)
        return scale

    def project(vf, start, stop, ready=()):
        rows = (stop - start) * rank
        @pl.when(spot >= 0)
        def _():
            totals = [jnp.zeros((leaves, rows), F32)] * 2
            for c in range(leaves):
                if ready and c % (leaves // PIECES) == 0:
                    ready[c // (leaves // PIECES)].wait()
                lhs = jnp.where(row == c, vf, 0.0).astype(BF16)
                rhs = right[start:stop, :, c * leaf:(c + 1) * leaf].reshape(rows, leaf)
                totals[c % 2] += dot(lhs, rhs, NT)
            for n in range(2):
                sums[n, :, :rows] = totals[n]

        return sums[0, :, :rows] + sums[1, :, :rows]

    def apply_far(total, weights, start, stop):
        rows = (stop - start) * rank
        row_w = lax.broadcasted_iota(jnp.int32, weights.shape, 0)

        @pl.when(spot >= 0)
        def _():
            totals = [jnp.zeros((leaves, leaf), F32)] * 2
            for i in range(leaves):
                lhs = jnp.where(row_w == i, weights, 0.0).astype(BF16)[:, :rows]
                rhs = left[start:stop, :, i * leaf:(i + 1) * leaf].reshape(rows, leaf)
                totals[i % 2] += dot(lhs, rhs, NN)
            for n in range(2):
                sums[n] = totals[n]

        return sums[0] + sums[1] if total is None else total + sums[0] + sums[1]

    def spread(mask, value):
        return jnp.where(masks[mask] > 0.0, jnp.broadcast_to(value, (leaves, LANES)), 0.0)

    def send(src, dst, send_sem, recv_sem, peer):
        pltpu.make_async_remote_copy(
            src_ref=src, dst_ref=dst, send_sem=send_sem, recv_sem=recv_sem, **target(peer)
        ).start()

    def rows_done(ref, rows, sem):
        part = ref.at[pl.ds(0, rows)]
        pltpu.make_async_copy(part, part, sem).wait()

    def write_mail(step, vf, ready=()):
        own[step] = vf.astype(BF16)
        summed = project(vf, high, levels, ready)
        device_sums = jnp.sum(summed, axis=0, keepdims=True)
        one = pltpu.roll(device_sums[:, :LANES], 2 * rank, 1)
        two = pltpu.roll(device_sums[:, LANES:], 2 * rank, 1)
        mail[step, 0] = jnp.where(lane1 < 2 * rank, one, two)
        mail[step, 1] = jnp.where(lane1 < 2 * rank, two, one)
        return summed[:, :rank]

    def send_halo(step, side):
        send(own.at[step], halo.at[step, side], halo_send.at[step, side], halo_recv.at[step, side],
             left_of if side else right_of)

    def wait_halo(step, sems):
        for side in range(2):
            pltpu.make_async_copy(own.at[step], own.at[step], sems.at[step, side]).wait()

    def far_slot(g, step, c):
        return g * plane + step * 2 + c

    def local_part(step, vf, last_local, pair):
        below = project(vf, 0, high)
        fine = jnp.concatenate([below, last_local], axis=1)
        chosen = jnp.zeros((leaves, LANES), F32)
        cluster_r = lax.broadcasted_iota(jnp.int32, (leaves, leaves), 0)
        cluster_c = lax.broadcasted_iota(jnp.int32, (leaves, leaves), 1)
        for level in range(local_levels):
            pick = (cluster_c >> level) == ((cluster_r >> level) ^ 1)
            partner = lax.dot_general(
                pick.astype(F32), fine, NN,
                precision=lax.Precision.HIGHEST, preferred_element_type=F32,
            )
            chosen = jnp.where(lane // rank == level, partner * scale_of(level), chosen)
        chosen = jnp.where(masks[0] > 0.0, chosen, 0.0)
        pair = pltpu.roll(spread(2, pair * scale_of(local_levels)), rank, 1)
        total = apply_far(None, jnp.concatenate([chosen, pair], axis=1), 0, local_levels + 1)
        wait_halo(step, halo_recv)
        extended = jnp.concatenate([halo[step, 0], own[step], halo[step, 1]], axis=0)
        leaf_no = lax.broadcasted_iota(jnp.int32, (3 * leaves, leaves), 0) + (me - 1) * leaves
        for k in range(nears):
            hot = jnp.broadcast_to(index[k:k + 1, :], (3 * leaves, leaves)) == leaf_no
            picks[k] = dot(hot.astype(F32).astype(BF16), extended, TN)

        def near_leaves(n, totals):
            totals = list(totals)
            for m in range(NEAR_UNROLL):
                i = n * NEAR_UNROLL + m
                for k in range(nears):
                    lhs = jnp.where(row == i, picks[k], 0.0).astype(BF16)
                    totals[m % 2] += dot(lhs, near[i, k], NT)
            return tuple(totals)

        totals = lax.fori_loop(
            0, leaves // NEAR_UNROLL, near_leaves, (total, jnp.zeros((leaves, leaf), F32))
        )
        return totals[0] + totals[1]

    ring_scale = by_lane([scale_of(local_levels + 1 + j) for j in range(ring_bits)])
    plane_scale = by_lane([scale_of(levels - 2), scale_of(levels - 1)])
    ring_levels = (local_levels + 1, local_levels + 1 + ring_bits)

    def finish(step, total):
        out[step, pl.ds(0, leaves, 2), :] = total[:, :LANES]
        out[step, pl.ds(1, leaves, 2), :] = total[:, LANES:]

    loads[0].wait()
    slip_rate = jnp.concatenate([slip[pl.ds(0, leaves, 2), :], slip[pl.ds(1, leaves, 2), :]], axis=1)
    vf = slip_rate.astype(BF16).astype(F32)
    last_local = write_mail(0, vf, pieces)
    pl.semaphore_wait(barrier, expected)
    for j in upper:
        @pl.when(bit(j) if j > quad_bits else jnp.logical_not(bit(j)))
        def _(j=j):
            pl.semaphore_signal(ready.at[j - quad_bits], inc=1, **target(peer_of(0, relay_step[j], 0)))

    pl.when(jnp.logical_not(bottom))(
        lambda: pl.semaphore_signal(near_ready.at[0], inc=1, **target(left_of)))
    pl.when(top)(lambda: pl.semaphore_signal(near_ready.at[1], inc=1, **target(right_of)))

    def send_letter(t, sem):
        send(mail.at[0], got.at[t], level_send.at[sem], level_recv.at[sem], jnp.bitwise_xor(me, t))

    for t in reversed(range(1, quad)):
        send_letter(t, 1)
    for j, first_step, stride, length in runs:
        if j > quad_bits:
            @pl.when(bit(j))
            def _(j=j, first_step=first_step, stride=stride, length=length):
                def both(step):
                    for c in range(2):
                        send_letter(step * 2 + c, 0)
                run(first_step, stride, length, both)
    pl.when(jnp.logical_not(top))(lambda: pl.semaphore_wait(near_ready.at[0], 1))
    send_halo(0, 0)
    pl.when(jnp.logical_not(bottom))(lambda: send_halo(0, 1))

    rows_done(got, quad - 1, level_recv.at[1])

    def sum_of(j, kind):
        return add_all(got[t, kind] for t in range(2 ** (j + 1), 2 ** (j + 2)))

    quad_ring = [sum_of(j, 0) for j in range(quad_bits)]
    known[0] = add_all([mail[0, 0], got[1, 0]] + quad_ring)
    known[1] = add_all([mail[0, 1], got[1, 1]] + [sum_of(j, 1) for j in range(quad_bits)])
    given = jnp.zeros((1, LANES), F32)
    for j in range(quad_bits):
        given = jnp.where(lane1 // rank == j, quad_ring[j], given)
    known[2] = given

    def take(j, ring_sum, far_sum):
        known[2] = jnp.where(lane1 // rank == j, ring_sum, known[2])
        known[0] = known[0] + ring_sum
        known[1] = known[1] + far_sum

    def settle_relay(n):
        part = got_relay.at[n]
        pltpu.make_async_copy(part, part, relay_recv.at[n]).wait()
        take(quad_bits + n, got_relay[n, 0], got_relay[n, 1])

    def send_relay(n):
        relay[n, 0] = known[0]
        relay[n, 1] = known[1]
        waits = jnp.logical_not(bit(quad_bits + n)) if n else bit(quad_bits)
        pl.when(waits)(lambda: pl.semaphore_wait(ready.at[n], 1))
        send(relay.at[n], got_relay.at[n], relay_send.at[n], relay_recv.at[n],
             peer_of(0, relay_step[quad_bits + n], 0))

    send_relay(0)
    low = jnp.logical_not(bit(ring_bits - 1))

    @pl.when(bottom)
    def _():
        pl.semaphore_wait(near_ready.at[1], 1)
        send_halo(0, 1)

    @pl.when(low)
    def _():
        settle_relay(0)
        send_relay(1)

    loads[2].wait()
    loads[3].wait()
    for group, held in enumerate((
        list(range(local_levels)), list(range(*ring_levels)),
        [levels - 2, levels - 1, None, local_levels],
    )):
        limit = jnp.zeros((leaves, LANES), jnp.int32)
        for part, level in enumerate(held):
            if level is not None:
                column = jnp.broadcast_to(ranks[:, level:level + 1], (leaves, LANES))
                limit = jnp.where(lane // rank == part, column, limit)
        masks[group] = (lane % rank < limit).astype(F32)
    for n in (4, 1, 5):
        loads[n].wait()
    total = local_part(0, vf, last_local, got[1, 1])
    @pl.when(jnp.logical_not(low))
    def _():
        settle_relay(0)
        settle_relay(1)

    @pl.when(low)
    def _():
        rows_done(got, ring, level_recv.at[0])
        take(ring_bits - 1, sum_of(ring_bits - 1, 0), sum_of(ring_bits - 1, 1))

    plane_sums[...] = known[1]
    for g in far_first[:-1]:
        send(plane_sums, got_plane.at[g], plane_send.at[0], plane_recv.at[0], peer_of(g, 0, 0))
    total = apply_far(total, spread(1, known[2] * ring_scale), *ring_levels)
    rows_done(got_plane, groups - 1, plane_recv.at[0])
    far_sum = jnp.where(lane1 < rank, got_plane[1], add_all(got_plane[g] for g in range(2, groups)))
    first = apply_far(total, spread(2, far_sum * plane_scale), levels - FAR_BITS, levels)
    finish(0, first)

    relaxed = slip_rate + jnp.tanh(first / 3.0)
    vf = relaxed.astype(BF16).astype(F32)
    last_local = write_mail(1, vf)
    def send_row(g, step, c):
        sem = 1 if g else 0
        slot = g * plane + step * 2 + c
        send(mail.at[1, sem], got_all.at[slot], all_send.at[sem], all_recv.at[sem], peer_of(g, step, c))

    for j, first_step, stride, length in runs:
        def all_of(step):
            for g in far_first:
                for c in range(2):
                    send_row(g, step, c)
        run(first_step, stride, length, all_of)
    for g in far_first[:-1]:
        for c in range(2):
            send_row(g, 0, c)
    send(mail.at[1, 1], got_pair, pair_send.at[0], pair_recv.at[0], peer_of(0, 0, 1))
    send_halo(1, 0)
    send_halo(1, 1)
    pltpu.make_async_copy(got_pair, got_pair, pair_recv.at[0]).wait()
    total = local_part(1, vf, last_local, got_pair[...])
    rows_done(got_all, plane - 2, all_recv.at[0])
    sibling = jnp.zeros((1, LANES), F32)
    for j in range(ring_bits):
        ring_sum = add_all(got_all[t] for t in range(2 ** (j + 1), 2 ** (j + 2)))
        sibling = jnp.where(lane1 // rank == j, ring_sum, sibling)
    total = apply_far(total, spread(1, sibling * ring_scale), *ring_levels)
    rows_done(got_all, count - plane, all_recv.at[1])
    far_sum = jnp.where(
        lane1 < rank, add_all(got_all[t] for t in range(plane, 2 * plane)),
        add_all(got_all[t] for t in range(2 * plane, count)),
    )
    finish(1, apply_far(total, spread(2, far_sum * plane_scale), levels - FAR_BITS, levels))

    for step in range(2):
        wait_halo(step, halo_send)
    rows_done(got, quad - 1, level_send.at[1])
    pltpu.make_async_copy(relay.at[0], relay.at[0], relay_send.at[0]).wait()

    @pl.when(low)
    def _():
        pltpu.make_async_copy(relay.at[1], relay.at[1], relay_send.at[1]).wait()

    @pl.when(jnp.logical_not(low))
    def _():
        rows_done(got, ring, level_send.at[0])

    rows_done(got_plane, groups - 1, plane_send.at[0])
    rows_done(got_all, plane - 2, all_send.at[0])
    rows_done(got_all, count - plane, all_send.at[1])
    pltpu.make_async_copy(got_pair, got_pair, pair_send.at[0]).wait()


def write(out, first, second, sem):
    copies = [pltpu.make_async_copy(out.at[n], ref, sem.at[n]) for n, ref in enumerate((first, second))]
    for copy in copies:
        copy.start()
    for copy in copies:
        copy.wait()


def local(count, slip_rate, near_blocks, near_index, far_left, far_right, far_ranks):
    leaves, nears, leaf, _ = near_blocks.shape
    levels, rank, patches = far_left.shape
    cross = levels - (leaves.bit_length() - 1)
    ring_bits = cross - FAR_BITS - 1
    plane = count // 2**FAR_BITS
    assert leaf == 2 * LANES and 4 * rank == LANES and 2**cross == count
    assert leaves == 16 and ring_bits == 4
    flat = (patches // LANES, LANES)
    anywhere = pl.BlockSpec(memory_space=pl.ANY)
    dma = pltpu.SemaphoreType.DMA
    out = pl.pallas_call(
        functools.partial(kernel, (count, leaves, nears, leaf, levels, rank)),
        out_shape=pltpu.VMEM((2,) + flat, F32),
        in_specs=[anywhere] * 6,
        out_specs=pl.BlockSpec(memory_space=pltpu.VMEM),
        scratch_shapes=[
            pltpu.VMEM(flat, F32),
            pltpu.VMEM(far_ranks.shape, jnp.int32),
            pltpu.VMEM(near_index.shape[::-1], jnp.int32),
            pltpu.VMEM(far_right.shape, BF16),
            pltpu.VMEM(near_blocks.shape, BF16),
            pltpu.VMEM(far_left.shape, BF16),
            pltpu.VMEM((2, leaves, leaf), BF16),
            pltpu.VMEM((2, 2, leaves, leaf), BF16),
            pltpu.VMEM((3, leaves, LANES), F32),
            pltpu.VMEM((nears, leaves, leaf), F32),
            pltpu.VMEM((2, leaves, leaf), F32),
            pltpu.VMEM((2, 2, 1, LANES), F32),
            pltpu.VMEM((plane, 2, 1, LANES), F32),
            pltpu.VMEM((3, 1, LANES), F32),
            pltpu.VMEM((2, 2, 1, LANES), F32),
            pltpu.VMEM((2, 2, 1, LANES), F32),
            pltpu.VMEM((1, LANES), F32),
            pltpu.VMEM((2**FAR_BITS, 1, LANES), F32),
            pltpu.VMEM((count, 1, LANES), F32),
            pltpu.VMEM((1, LANES), F32),
            dma((6,)), dma((PIECES,)), dma((2, 2)), dma((2, 2)),
            dma((2,)), dma((2,)), dma((2,)), dma((2,)),
            dma((1,)), dma((1,)), dma((2,)), dma((2,)), dma((1,)), dma((1,)),
            pltpu.SemaphoreType.REGULAR((2,)), pltpu.SemaphoreType.REGULAR((2,)),
        ],
        compiler_params=pltpu.CompilerParams(collective_id=0, has_side_effects=True),
        name="hmatrix",
    )(slip_rate.reshape(flat), far_ranks, near_index.T, far_right, near_blocks, far_left)
    first, second = pl.pallas_call(
        write,
        out_shape=[jax.ShapeDtypeStruct(flat, F32)] * 2,
        in_specs=[pl.BlockSpec(memory_space=pltpu.VMEM)],
        out_specs=[anywhere] * 2,
        scratch_shapes=[dma((2,))],
        name="write",
    )(pltpu.with_memory_space_constraint(out, pltpu.VMEM))
    return first.reshape(-1), second.reshape(-1)


def solution(mesh):
    both = ("models", "leaf")
    in_specs = (
        P(both), P(both, None, None, None), P(both, None),
        P(None, None, both), P(None, None, both), P(both, None),
    )
    return jax.shard_map(
        functools.partial(local, mesh.shape["leaf"]), mesh=mesh, in_specs=in_specs,
        out_specs=(P(both), P(both)), check_vma=False,
    )
```

```python
import functools
import math

import jax
import jax.numpy as jnp
from jax import lax
from jax.experimental import pallas as pl
from jax.experimental.pallas import tpu as pltpu
from jax.sharding import PartitionSpec as P

MESH = pl.DeviceIdType.MESH
F32 = jnp.float32
BF16 = jnp.bfloat16
LANES = 128
FAR_BITS = 2
PIECES = 4
NEAR_UNROLL = 4
NT = (((1,), (1,)), ((), ()))
NN = (((1,), (0,)), ((), ()))
TN = (((0,), (0,)), ((), ()))


def dot(a, b, dims):
    return lax.dot_general(a, b, dims, preferred_element_type=F32)


def add_all(terms):
    terms = list(terms)
    while len(terms) > 1:
        odd = terms[len(terms) // 2 * 2:]
        terms = [x + y for x, y in zip(terms[::2], terms[1::2])] + odd
    return terms[0]


def kernel(
    shape,
    slip_hbm, ranks_hbm, index_hbm, right_hbm, near_hbm, left_hbm,
    out,
    slip, ranks, index, right, near, left, own, halo, masks, picks, sums, partial,
    mail, got, known, relay, got_relay, plane_sums, got_plane, got_all, got_pair,
    load_sem, piece_sem, halo_send, halo_recv, level_send, level_recv, relay_send, relay_recv,
    plane_send, plane_recv, all_send, all_recv, pair_send, pair_recv, ready, near_ready, plane_ready,
):
    count, leaves, nears, leaf, levels, rank = shape
    local_levels = leaves.bit_length() - 1
    cross = levels - local_levels
    groups = 2**FAR_BITS
    plane = count // groups
    ring_bits = cross - FAR_BITS - 1
    ring = 2**ring_bits
    me = lax.axis_index("leaf")
    spot = lax.rem(me // 2, ring)

    def peer_of(far, step, core):
        return jnp.bitwise_xor(me, far * plane + step * 2 + core)

    def bit(j):
        return lax.rem(spot // 2**j, 2) == 1

    def target(peer):
        return dict(device_id={"leaf": peer}, device_id_type=MESH)

    right_of = lax.rem(me + 1, count)
    left_of = lax.rem(me + count - 1, count)
    far_first = [g for g in (2, 3, 1, 0) if g < groups]
    quad_bits = ring_bits - 2
    quad = 2 ** (quad_bits + 1)
    upper = range(quad_bits, ring_bits)
    relay_step = {quad_bits: ring // 4, quad_bits + 1: ring // 2 + ring // 4}
    half = ring // 2
    runs = [(ring_bits - 1, half, 1, half // 2), (ring_bits - 2, half - 1, -1, half // 2),
            (ring_bits - 1, half + half // 2, 1, half // 2)]
    runs += [(j, 2 ** (j + 1) - 1, -1, 2**j) for j in reversed(range(ring_bits - 2))]

    def run(first, stride, length, body):
        def trip(n, carry):
            body(first + stride * n)
            return carry

        lax.fori_loop(0, length, trip, 0)

    high = local_levels - 1
    piece = leaves // PIECES * leaf
    loads = [
        pltpu.make_async_copy(slip_hbm, slip, load_sem.at[0]),
        pltpu.make_async_copy(left_hbm, left, load_sem.at[1]),
        pltpu.make_async_copy(ranks_hbm, ranks, load_sem.at[2]),
        pltpu.make_async_copy(index_hbm, index, load_sem.at[3]),
        pltpu.make_async_copy(right_hbm.at[pl.ds(0, high)], right.at[pl.ds(0, high)], load_sem.at[4]),
        pltpu.make_async_copy(near_hbm, near, load_sem.at[5]),
    ]
    pieces = []
    for n in range(PIECES):
        part = (pl.ds(high, levels - high), slice(None), pl.ds(n * piece, piece))
        pieces.append(pltpu.make_async_copy(right_hbm.at[part], right.at[part], piece_sem.at[n]))
    loads[0].start()
    for load in pieces:
        load.start()

    barrier = pltpu.get_barrier_semaphore()

    def greet(peer):
        pl.semaphore_signal(barrier, inc=1, **target(peer))

    low = jnp.logical_not(bit(ring_bits - 1))
    outer = bit(ring_bits - 1) == bit(quad_bits)
    inner = jnp.logical_not(outer)
    plane_no = me // plane

    def plane_above(g):
        return lax.rem(plane_no // 2 ** (g.bit_length() - 1), 2) == 1

    for j, first_step, stride, length in runs:
        if j > quad_bits:
            @pl.when(low)
            def _(first_step=first_step, stride=stride, length=length):
                def both(step):
                    for c in range(2):
                        greet(peer_of(0, step, c))
                run(first_step, stride, length, both)
    expected = quad - 1
    for t in reversed(range(1, quad)):
        greet(peer_of(0, t // 2, t % 2))
    for g in far_first[:-1]:
        pl.when(plane_above(g))(lambda g=g: greet(peer_of(g, 0, 0)))
        expected = expected + jnp.where(plane_above(g), 0, 1)
    @pl.when(inner)
    def _():
        for t in reversed(range(quad, 2 * quad)):
            greet(peer_of(0, t // 2, t % 2))

    expected = expected + jnp.where(outer, quad, 0)
    expected = expected + jnp.where(low, 0, ring)
    top = jnp.logical_and(spot == ring - 1, lax.rem(me, 2) == 1)
    bottom = jnp.logical_and(spot == 0, lax.rem(me, 2) == 0)
    pl.when(jnp.logical_not(top))(lambda: greet(right_of))
    pl.when(bottom)(lambda: greet(left_of))
    expected = expected + jnp.where(bottom, 0, 1) + jnp.where(top, 1, 0)
    for load in (loads[2], loads[3], loads[4], loads[1], loads[5]):
        load.start()

    row = lax.broadcasted_iota(jnp.int32, (leaves, leaf), 0)
    row_l = lax.broadcasted_iota(jnp.int32, (leaves, LANES), 0)
    lane = lax.broadcasted_iota(jnp.int32, (leaves, LANES), 1)
    lane1 = lax.broadcasted_iota(jnp.int32, (1, LANES), 1)

    def scale_of(level):
        return 1.0 / math.sqrt(leaf * 2**level)

    def by_lane(values):
        scale = jnp.zeros((1, LANES), F32)
        for part, value in enumerate(values):
            scale = jnp.where(lane1 // rank == part, value, scale)
        return scale

    def project(vf, start, stop, ready=()):
        rows = (stop - start) * rank
        @pl.when(spot >= 0)
        def _():
            totals = [jnp.zeros((leaves, rows), F32)] * 2
            for c in range(leaves):
                if ready and c % (leaves // PIECES) == 0:
                    ready[c // (leaves // PIECES)].wait()
                lhs = jnp.where(row == c, vf, 0.0).astype(BF16)
                rhs = right[start:stop, :, c * leaf:(c + 1) * leaf].reshape(rows, leaf)
                totals[c % 2] += dot(lhs, rhs, NT)
            for n in range(2):
                sums[n, :, :rows] = totals[n]

        return sums[0, :, :rows] + sums[1, :, :rows]

    def apply_far(total, weights, start, stop):
        rows = (stop - start) * rank
        row_w = lax.broadcasted_iota(jnp.int32, weights.shape, 0)

        @pl.when(spot >= 0)
        def _():
            totals = [jnp.zeros((leaves, leaf), F32)] * 2
            for i in range(leaves):
                lhs = jnp.where(row_w == i, weights, 0.0).astype(BF16)[:, :rows]
                rhs = left[start:stop, :, i * leaf:(i + 1) * leaf].reshape(rows, leaf)
                totals[i % 2] += dot(lhs, rhs, NN)
            for n in range(2):
                sums[n] = totals[n]

        return sums[0] + sums[1] if total is None else total + sums[0] + sums[1]

    def spread(mask, value):
        return jnp.where(masks[mask] > 0.0, jnp.broadcast_to(value, (leaves, LANES)), 0.0)

    def send(src, dst, send_sem, recv_sem, peer):
        pltpu.make_async_remote_copy(
            src_ref=src, dst_ref=dst, send_sem=send_sem, recv_sem=recv_sem, **target(peer)
        ).start()

    def rows_done(ref, rows, sem):
        part = ref.at[pl.ds(0, rows)]
        pltpu.make_async_copy(part, part, sem).wait()

    def write_mail(step, vf, ready=()):
        own[step] = vf.astype(BF16)
        summed = project(vf, high, levels, ready)
        device_sums = jnp.sum(summed, axis=0, keepdims=True)
        one = pltpu.roll(device_sums[:, :LANES], 2 * rank, 1)
        two = pltpu.roll(device_sums[:, LANES:], 2 * rank, 1)
        mail[step, 0] = jnp.where(lane1 < 2 * rank, one, two)
        mail[step, 1] = jnp.where(lane1 < 2 * rank, two, one)
        return summed[:, :rank]

    def send_halo(step, side):
        send(own.at[step], halo.at[step, side], halo_send.at[step, side], halo_recv.at[step, side],
             left_of if side else right_of)

    def wait_halo(step, sems):
        for side in range(2):
            pltpu.make_async_copy(own.at[step], own.at[step], sems.at[step, side]).wait()

    def far_slot(g, step, c):
        return g * plane + step * 2 + c

    def local_part(step, vf, last_local):
        below = project(vf, 0, high)
        fine = jnp.concatenate([below, last_local], axis=1)
        chosen = jnp.zeros((leaves, LANES), F32)
        cluster_r = lax.broadcasted_iota(jnp.int32, (leaves, leaves), 0)
        cluster_c = lax.broadcasted_iota(jnp.int32, (leaves, leaves), 1)
        for level in range(local_levels):
            pick = (cluster_c >> level) == ((cluster_r >> level) ^ 1)
            partner = lax.dot_general(
                pick.astype(F32), fine, NN,
                precision=lax.Precision.HIGHEST, preferred_element_type=F32,
            )
            chosen = jnp.where(lane // rank == level, partner * scale_of(level), chosen)
        chosen = jnp.where(masks[0] > 0.0, chosen, 0.0)
        total = apply_far(None, chosen, 0, local_levels)
        wait_halo(step, halo_recv)
        extended = jnp.concatenate([halo[step, 0], own[step], halo[step, 1]], axis=0)
        leaf_no = lax.broadcasted_iota(jnp.int32, (3 * leaves, leaves), 0) + (me - 1) * leaves
        for k in range(nears):
            hot = jnp.broadcast_to(index[k:k + 1, :], (3 * leaves, leaves)) == leaf_no
            picks[k] = dot(hot.astype(F32).astype(BF16), extended, TN)

        def near_leaves(n, totals):
            totals = list(totals)
            for m in range(NEAR_UNROLL):
                i = n * NEAR_UNROLL + m
                for k in range(nears):
                    lhs = jnp.where(row == i, picks[k], 0.0).astype(BF16)
                    totals[m % 2] += dot(lhs, near[i, k], NT)
            return tuple(totals)

        totals = lax.fori_loop(
            0, leaves // NEAR_UNROLL, near_leaves, (total, jnp.zeros((leaves, leaf), F32))
        )
        partial[...] = totals[0] + totals[1]

    def apply_ring(pair, siblings):
        pair = pltpu.roll(spread(2, pair * scale_of(local_levels)), rank, 1)
        moved = pltpu.roll(spread(1, siblings * ring_scale), rank, 1)
        weights = jnp.concatenate([jnp.where(lane < rank, pair, moved), moved], axis=1)
        return apply_far(partial[...], weights, local_levels, local_levels + 1 + ring_bits)

    ring_scale = by_lane([scale_of(local_levels + 1 + j) for j in range(ring_bits)])
    plane_scale = by_lane([scale_of(levels - 2), scale_of(levels - 1)])
    ring_levels = (local_levels + 1, local_levels + 1 + ring_bits)

    def finish(step, total):
        out[step, pl.ds(0, leaves, 2), :] = total[:, :LANES]
        out[step, pl.ds(1, leaves, 2), :] = total[:, LANES:]

    def meet():
        pl.semaphore_wait(barrier, expected)
        for j in upper:
            @pl.when(bit(j) if j > quad_bits else outer)
            def _(j=j):
                pl.semaphore_signal(ready.at[j - quad_bits], inc=1, **target(peer_of(0, relay_step[j], 0)))

        for g in far_first[:-1]:
            pl.when(jnp.logical_not(plane_above(g)))(
                lambda g=g: pl.semaphore_signal(plane_ready.at[g], inc=1, **target(peer_of(g, 0, 0))))
        pl.when(jnp.logical_not(bottom))(
            lambda: pl.semaphore_signal(near_ready.at[0], inc=1, **target(left_of)))
        pl.when(top)(lambda: pl.semaphore_signal(near_ready.at[1], inc=1, **target(right_of)))

    last = spot == ring - 1
    late = spot >= ring - ring // 4
    pl.when(last)(meet)
    loads[0].wait()
    slip_rate = jnp.concatenate([slip[pl.ds(0, leaves, 2), :], slip[pl.ds(1, leaves, 2), :]], axis=1)
    vf = slip_rate.astype(BF16).astype(F32)
    last_local = write_mail(0, vf, pieces)
    pl.when(jnp.logical_not(last))(meet)
    def send_letter(t, sem):
        send(mail.at[0], got.at[t], level_send.at[sem], level_recv.at[sem], jnp.bitwise_xor(me, t))

    for t in reversed(range(1, quad)):
        send_letter(t, 1)
    @pl.when(outer)
    def _():
        for t in reversed(range(quad, 2 * quad)):
            send_letter(t, 2)

    for j, first_step, stride, length in runs:
        if j > quad_bits:
            @pl.when(bit(j))
            def _(j=j, first_step=first_step, stride=stride, length=length):
                def both(step):
                    for c in range(2):
                        send_letter(step * 2 + c, 0)
                run(first_step, stride, length, both)
    pl.when(jnp.logical_not(top))(lambda: pl.semaphore_wait(near_ready.at[0], 1))
    send_halo(0, 0)
    pl.when(jnp.logical_not(bottom))(lambda: send_halo(0, 1))

    def own_work():
        loads[2].wait()
        loads[3].wait()
        for group, held in enumerate((
            list(range(local_levels)), list(range(*ring_levels)),
            [levels - 2, levels - 1, None, local_levels],
        )):
            limit = jnp.zeros((leaves, LANES), jnp.int32)
            for part, level in enumerate(held):
                if level is not None:
                    column = jnp.broadcast_to(ranks[:, level:level + 1], (leaves, LANES))
                    limit = jnp.where(lane // rank == part, column, limit)
            masks[group] = (lane % rank < limit).astype(F32)
        for n in (4, 1, 5):
            loads[n].wait()
        local_part(0, vf, last_local)

    pl.when(late)(own_work)

    rows_done(got, quad - 1, level_recv.at[1])

    def sum_of(j, kind):
        return add_all(got[t, kind] for t in range(2 ** (j + 1), 2 ** (j + 2)))

    quad_ring = [sum_of(j, 0) for j in range(quad_bits)]
    known[0] = add_all([mail[0, 0], got[1, 0]] + quad_ring)
    known[1] = add_all([mail[0, 1], got[1, 1]] + [sum_of(j, 1) for j in range(quad_bits)])
    given = jnp.zeros((1, LANES), F32)
    for j in range(quad_bits):
        given = jnp.where(lane1 // rank == j, quad_ring[j], given)
    known[2] = given

    def take(j, ring_sum, far_sum):
        known[2] = jnp.where(lane1 // rank == j, ring_sum, known[2])
        known[0] = known[0] + ring_sum
        known[1] = known[1] + far_sum

    def settle_relay(n):
        part = got_relay.at[n]
        pltpu.make_async_copy(part, part, relay_recv.at[n]).wait()
        take(quad_bits + n, got_relay[n, 0], got_relay[n, 1])

    def send_relay(n):
        relay[n, 0] = known[0]
        relay[n, 1] = known[1]
        pl.semaphore_wait(ready.at[n], 1)
        send(relay.at[n], got_relay.at[n], relay_send.at[n], relay_recv.at[n],
             peer_of(0, relay_step[quad_bits + n], 0))

    pl.when(inner)(lambda: send_relay(0))

    @pl.when(bottom)
    def _():
        pl.semaphore_wait(near_ready.at[1], 1)
        send_halo(0, 1)

    def settle_half():
        pl.when(outer)(lambda: settle_relay(0))

        @pl.when(inner)
        def _():
            rows_done(got, quad, level_recv.at[2])
            take(quad_bits, sum_of(quad_bits, 0), sum_of(quad_bits, 1))

    @pl.when(low)
    def _():
        settle_half()
        send_relay(1)

    pl.when(jnp.logical_not(late))(own_work)
    @pl.when(jnp.logical_not(low))
    def _():
        settle_half()
        settle_relay(1)

    @pl.when(low)
    def _():
        rows_done(got, ring, level_recv.at[0])
        take(ring_bits - 1, sum_of(ring_bits - 1, 0), sum_of(ring_bits - 1, 1))

    plane_sums[...] = known[1]
    for g in far_first[:-1]:
        pl.when(plane_above(g))(lambda g=g: pl.semaphore_wait(plane_ready.at[g], 1))
        send(plane_sums, got_plane.at[g], plane_send.at[0], plane_recv.at[0], peer_of(g, 0, 0))
    total = apply_ring(got[1, 1], known[2])
    rows_done(got_plane, groups - 1, plane_recv.at[0])
    far_sum = jnp.where(lane1 < rank, got_plane[1], add_all(got_plane[g] for g in range(2, groups)))
    first = apply_far(total, spread(2, far_sum * plane_scale), levels - FAR_BITS, levels)
    finish(0, first)

    relaxed = slip_rate + jnp.tanh(first / 3.0)
    vf = relaxed.astype(BF16).astype(F32)
    last_local = write_mail(1, vf)
    def send_row(g, step, c):
        sem = 1 if g else 0
        slot = g * plane + step * 2 + c
        send(mail.at[1, sem], got_all.at[slot], all_send.at[sem], all_recv.at[sem], peer_of(g, step, c))

    for j, first_step, stride, length in runs:
        def all_of(step):
            for g in far_first:
                for c in range(2):
                    send_row(g, step, c)
        run(first_step, stride, length, all_of)
    for g in far_first[:-1]:
        for c in range(2):
            send_row(g, 0, c)
    send(mail.at[1, 1], got_pair, pair_send.at[0], pair_recv.at[0], peer_of(0, 0, 1))
    send_halo(1, 0)
    send_halo(1, 1)
    local_part(1, vf, last_local)
    pltpu.make_async_copy(got_pair, got_pair, pair_recv.at[0]).wait()
    rows_done(got_all, plane - 2, all_recv.at[0])
    sibling = jnp.zeros((1, LANES), F32)
    for j in range(ring_bits):
        ring_sum = add_all(got_all[t] for t in range(2 ** (j + 1), 2 ** (j + 2)))
        sibling = jnp.where(lane1 // rank == j, ring_sum, sibling)
    total = apply_ring(got_pair[...], sibling)
    rows_done(got_all, count - plane, all_recv.at[1])
    far_sum = jnp.where(
        lane1 < rank, add_all(got_all[t] for t in range(plane, 2 * plane)),
        add_all(got_all[t] for t in range(2 * plane, count)),
    )
    finish(1, apply_far(total, spread(2, far_sum * plane_scale), levels - FAR_BITS, levels))

    for step in range(2):
        wait_halo(step, halo_send)
    rows_done(got, quad - 1, level_send.at[1])
    pl.when(inner)(
        lambda: pltpu.make_async_copy(relay.at[0], relay.at[0], relay_send.at[0]).wait())
    pl.when(outer)(lambda: rows_done(got, quad, level_send.at[2]))

    @pl.when(low)
    def _():
        pltpu.make_async_copy(relay.at[1], relay.at[1], relay_send.at[1]).wait()

    @pl.when(jnp.logical_not(low))
    def _():
        rows_done(got, ring, level_send.at[0])

    rows_done(got_plane, groups - 1, plane_send.at[0])
    rows_done(got_all, plane - 2, all_send.at[0])
    rows_done(got_all, count - plane, all_send.at[1])
    pltpu.make_async_copy(got_pair, got_pair, pair_send.at[0]).wait()


def write(out, first, second, sem):
    copies = [pltpu.make_async_copy(out.at[n], ref, sem.at[n]) for n, ref in enumerate((first, second))]
    for copy in copies:
        copy.start()
    for copy in copies:
        copy.wait()


def local(count, slip_rate, near_blocks, near_index, far_left, far_right, far_ranks):
    leaves, nears, leaf, _ = near_blocks.shape
    levels, rank, patches = far_left.shape
    cross = levels - (leaves.bit_length() - 1)
    ring_bits = cross - FAR_BITS - 1
    plane = count // 2**FAR_BITS
    assert leaf == 2 * LANES and 4 * rank == LANES and 2**cross == count
    assert leaves == 16 and ring_bits == 4
    flat = (patches // LANES, LANES)
    anywhere = pl.BlockSpec(memory_space=pl.ANY)
    dma = pltpu.SemaphoreType.DMA
    out = pl.pallas_call(
        functools.partial(kernel, (count, leaves, nears, leaf, levels, rank)),
        out_shape=pltpu.VMEM((2,) + flat, F32),
        in_specs=[anywhere] * 6,
        out_specs=pl.BlockSpec(memory_space=pltpu.VMEM),
        scratch_shapes=[
            pltpu.VMEM(flat, F32),
            pltpu.VMEM(far_ranks.shape, jnp.int32),
            pltpu.VMEM(near_index.shape[::-1], jnp.int32),
            pltpu.VMEM(far_right.shape, BF16),
            pltpu.VMEM(near_blocks.shape, BF16),
            pltpu.VMEM(far_left.shape, BF16),
            pltpu.VMEM((2, leaves, leaf), BF16),
            pltpu.VMEM((2, 2, leaves, leaf), BF16),
            pltpu.VMEM((3, leaves, LANES), F32),
            pltpu.VMEM((nears, leaves, leaf), F32),
            pltpu.VMEM((2, leaves, leaf), F32),
            pltpu.VMEM((leaves, leaf), F32),
            pltpu.VMEM((2, 2, 1, LANES), F32),
            pltpu.VMEM((plane, 2, 1, LANES), F32),
            pltpu.VMEM((3, 1, LANES), F32),
            pltpu.VMEM((2, 2, 1, LANES), F32),
            pltpu.VMEM((2, 2, 1, LANES), F32),
            pltpu.VMEM((1, LANES), F32),
            pltpu.VMEM((2**FAR_BITS, 1, LANES), F32),
            pltpu.VMEM((count, 1, LANES), F32),
            pltpu.VMEM((1, LANES), F32),
            dma((6,)), dma((PIECES,)), dma((2, 2)), dma((2, 2)),
            dma((3,)), dma((3,)), dma((2,)), dma((2,)),
            dma((1,)), dma((1,)), dma((2,)), dma((2,)), dma((1,)), dma((1,)),
            pltpu.SemaphoreType.REGULAR((2,)), pltpu.SemaphoreType.REGULAR((2,)),
            pltpu.SemaphoreType.REGULAR((2**FAR_BITS,)),
        ],
        compiler_params=pltpu.CompilerParams(collective_id=0, has_side_effects=True),
        name="hmatrix",
    )(slip_rate.reshape(flat), far_ranks, near_index.T, far_right, near_blocks, far_left)
    first, second = pl.pallas_call(
        write,
        out_shape=[jax.ShapeDtypeStruct(flat, F32)] * 2,
        in_specs=[pl.BlockSpec(memory_space=pltpu.VMEM)],
        out_specs=[anywhere] * 2,
        scratch_shapes=[dma((2,))],
        name="write",
    )(pltpu.with_memory_space_constraint(out, pltpu.VMEM))
    return first.reshape(-1), second.reshape(-1)


def solution(mesh):
    both = ("models", "leaf")
    in_specs = (
        P(both), P(both, None, None, None), P(both, None),
        P(None, None, both), P(None, None, both), P(both, None),
    )
    return jax.shard_map(
        functools.partial(local, mesh.shape["leaf"]), mesh=mesh, in_specs=in_specs,
        out_specs=(P(both), P(both)), check_vma=False,
    )
```

```python
import functools
import math

import jax
import jax.numpy as jnp
from jax import lax
from jax.experimental import pallas as pl
from jax.experimental.pallas import tpu as pltpu
from jax.sharding import PartitionSpec as P

MESH = pl.DeviceIdType.MESH
F32 = jnp.float32
BF16 = jnp.bfloat16
LANES = 128
FAR_BITS = 2
PIECES = 4
NEAR_UNROLL = 4
NT = (((1,), (1,)), ((), ()))
NN = (((1,), (0,)), ((), ()))
TN = (((0,), (0,)), ((), ()))


def dot(a, b, dims):
    return lax.dot_general(a, b, dims, preferred_element_type=F32)


def add_all(terms):
    terms = list(terms)
    while len(terms) > 1:
        odd = terms[len(terms) // 2 * 2:]
        terms = [x + y for x, y in zip(terms[::2], terms[1::2])] + odd
    return terms[0]


def kernel(
    shape,
    slip_hbm, ranks_hbm, index_hbm, right_hbm, near_hbm, left_hbm,
    out,
    slip, ranks, index, right, near, left, own, halo, masks, picks, sums, partial, turned,
    mail, got, known, relay, got_relay, plane_sums, got_plane, got_all, got_pair,
    load_sem, piece_sem, halo_send, halo_recv, level_send, level_recv, relay_send, relay_recv,
    plane_send, plane_recv, all_send, all_recv, pair_send, pair_recv, ready, near_ready, plane_ready,
):
    count, leaves, nears, leaf, levels, rank = shape
    local_levels = leaves.bit_length() - 1
    cross = levels - local_levels
    groups = 2**FAR_BITS
    plane = count // groups
    ring_bits = cross - FAR_BITS - 1
    ring = 2**ring_bits
    me = lax.axis_index("leaf")
    spot = lax.rem(me // 2, ring)

    def peer_of(far, step, core):
        return jnp.bitwise_xor(me, far * plane + step * 2 + core)

    def bit(j):
        return lax.rem(spot // 2**j, 2) == 1

    def target(peer):
        return dict(device_id={"leaf": peer}, device_id_type=MESH)

    right_of = lax.rem(me + 1, count)
    left_of = lax.rem(me + count - 1, count)
    far_first = [g for g in (2, 3, 1, 0) if g < groups]
    quad_bits = ring_bits - 2
    quad = 2 ** (quad_bits + 1)
    upper = range(quad_bits, ring_bits)
    relay_step = {quad_bits: ring // 4, quad_bits + 1: ring // 2 + ring // 4}
    half = ring // 2
    runs = [(ring_bits - 1, half, 1, half // 2), (ring_bits - 2, half - 1, -1, half // 2),
            (ring_bits - 1, half + half // 2, 1, half // 2)]
    runs += [(j, 2 ** (j + 1) - 1, -1, 2**j) for j in reversed(range(ring_bits - 2))]

    def run(first, stride, length, body):
        def trip(n, carry):
            body(first + stride * n)
            return carry

        lax.fori_loop(0, length, trip, 0)

    high = local_levels - 1
    piece = leaves // PIECES * leaf
    loads = [
        pltpu.make_async_copy(slip_hbm, slip, load_sem.at[0]),
        pltpu.make_async_copy(left_hbm, left, load_sem.at[1]),
        pltpu.make_async_copy(ranks_hbm, ranks, load_sem.at[2]),
        pltpu.make_async_copy(index_hbm, index, load_sem.at[3]),
        pltpu.make_async_copy(right_hbm.at[pl.ds(0, high)], right.at[pl.ds(0, high)], load_sem.at[4]),
        pltpu.make_async_copy(near_hbm, near, load_sem.at[5]),
    ]
    pieces = []
    for n in range(PIECES):
        part = (pl.ds(high, levels - high), slice(None), pl.ds(n * piece, piece))
        pieces.append(pltpu.make_async_copy(right_hbm.at[part], right.at[part], piece_sem.at[n]))
    loads[0].start()
    for load in pieces:
        load.start()

    barrier = pltpu.get_barrier_semaphore()

    def greet(peer):
        pl.semaphore_signal(barrier, inc=1, **target(peer))

    low = jnp.logical_not(bit(ring_bits - 1))
    outer = bit(ring_bits - 1) == bit(quad_bits)
    inner = jnp.logical_not(outer)
    plane_no = me // plane

    def plane_above(g):
        return lax.rem(plane_no // 2 ** (g.bit_length() - 1), 2) == 1

    for j, first_step, stride, length in runs:
        if j > quad_bits:
            @pl.when(low)
            def _(first_step=first_step, stride=stride, length=length):
                def both(step):
                    for c in range(2):
                        greet(peer_of(0, step, c))
                run(first_step, stride, length, both)
    expected = quad - 1
    for t in reversed(range(1, quad)):
        greet(peer_of(0, t // 2, t % 2))
    for g in far_first[:-1]:
        pl.when(plane_above(g))(lambda g=g: greet(peer_of(g, 0, 0)))
        expected = expected + jnp.where(plane_above(g), 0, 1)
    @pl.when(inner)
    def _():
        for t in reversed(range(quad, 2 * quad)):
            greet(peer_of(0, t // 2, t % 2))

    expected = expected + jnp.where(outer, quad, 0)
    expected = expected + jnp.where(low, 0, ring)
    top = jnp.logical_and(spot == ring - 1, lax.rem(me, 2) == 1)
    bottom = jnp.logical_and(spot == 0, lax.rem(me, 2) == 0)
    pl.when(jnp.logical_not(top))(lambda: greet(right_of))
    pl.when(bottom)(lambda: greet(left_of))
    expected = expected + jnp.where(bottom, 0, 1) + jnp.where(top, 1, 0)
    for load in (loads[2], loads[3], loads[4], loads[1], loads[5]):
        load.start()

    row = lax.broadcasted_iota(jnp.int32, (leaves, leaf), 0)
    row_l = lax.broadcasted_iota(jnp.int32, (leaves, LANES), 0)
    lane = lax.broadcasted_iota(jnp.int32, (leaves, LANES), 1)
    lane1 = lax.broadcasted_iota(jnp.int32, (1, LANES), 1)

    def scale_of(level):
        return 1.0 / math.sqrt(leaf * 2**level)

    def by_lane(values):
        scale = jnp.zeros((1, LANES), F32)
        for part, value in enumerate(values):
            scale = jnp.where(lane1 // rank == part, value, scale)
        return scale

    def turn():
        r = lax.broadcasted_iota(jnp.int32, (leaf, leaf), 0)
        eye = (r == lax.broadcasted_iota(jnp.int32, (leaf, leaf), 1)).astype(F32).astype(BF16)

        def pair_of(n, carry):
            for m in range(2):
                c = n * 2 + m
                block = right[high:levels, :, pl.ds(pl.multiple_of(c * leaf, leaf), leaf)]
                turned[c] = dot(eye, block.reshape(leaf, leaf), NT).astype(BF16)
            return carry

        lax.fori_loop(0, leaves // 2, pair_of, 0)

    def project_turned(vf):
        @pl.when(spot >= 0)
        def _():
            totals = [jnp.zeros((leaves, leaf), F32)] * 2
            for c in range(leaves):
                lhs = jnp.where(row == c, vf, 0.0).astype(BF16)
                totals[c % 2] += dot(lhs, turned[c], NN)
            for n in range(2):
                sums[n] = totals[n]

        return sums[0] + sums[1]

    def project(vf, start, stop, ready=()):
        rows = (stop - start) * rank
        @pl.when(spot >= 0)
        def _():
            totals = [jnp.zeros((leaves, rows), F32)] * 2
            for c in range(leaves):
                if ready and c % (leaves // PIECES) == 0:
                    ready[c // (leaves // PIECES)].wait()
                lhs = jnp.where(row == c, vf, 0.0).astype(BF16)
                rhs = right[start:stop, :, c * leaf:(c + 1) * leaf].reshape(rows, leaf)
                totals[c % 2] += dot(lhs, rhs, NT)
            for n in range(2):
                sums[n, :, :rows] = totals[n]

        return sums[0, :, :rows] + sums[1, :, :rows]

    def apply_far(total, weights, start, stop):
        rows = (stop - start) * rank
        row_w = lax.broadcasted_iota(jnp.int32, weights.shape, 0)

        @pl.when(spot >= 0)
        def _():
            totals = [jnp.zeros((leaves, leaf), F32)] * 2
            for i in range(leaves):
                lhs = jnp.where(row_w == i, weights, 0.0).astype(BF16)[:, :rows]
                rhs = left[start:stop, :, i * leaf:(i + 1) * leaf].reshape(rows, leaf)
                totals[i % 2] += dot(lhs, rhs, NN)
            for n in range(2):
                sums[n] = totals[n]

        return sums[0] + sums[1] if total is None else total + sums[0] + sums[1]

    def spread(mask, value):
        return jnp.where(masks[mask] > 0.0, jnp.broadcast_to(value, (leaves, LANES)), 0.0)

    def send(src, dst, send_sem, recv_sem, peer):
        pltpu.make_async_remote_copy(
            src_ref=src, dst_ref=dst, send_sem=send_sem, recv_sem=recv_sem, **target(peer)
        ).start()

    def rows_done(ref, rows, sem):
        part = ref.at[pl.ds(0, rows)]
        pltpu.make_async_copy(part, part, sem).wait()

    def write_mail(step, vf, ready=()):
        own[step] = vf.astype(BF16)
        summed = project_turned(vf) if step else project(vf, high, levels, ready)
        device_sums = jnp.sum(summed, axis=0, keepdims=True)
        one = pltpu.roll(device_sums[:, :LANES], 2 * rank, 1)
        two = pltpu.roll(device_sums[:, LANES:], 2 * rank, 1)
        mail[step, 0] = jnp.where(lane1 < 2 * rank, one, two)
        mail[step, 1] = jnp.where(lane1 < 2 * rank, two, one)
        return summed[:, :rank]

    def send_halo(step, side):
        send(own.at[step], halo.at[step, side], halo_send.at[step, side], halo_recv.at[step, side],
             left_of if side else right_of)

    def wait_halo(step, sems):
        for side in range(2):
            pltpu.make_async_copy(own.at[step], own.at[step], sems.at[step, side]).wait()

    def far_slot(g, step, c):
        return g * plane + step * 2 + c

    def local_part(step, vf, last_local):
        below = project(vf, 0, high)
        fine = jnp.concatenate([below, last_local], axis=1)
        chosen = jnp.zeros((leaves, LANES), F32)
        cluster_r = lax.broadcasted_iota(jnp.int32, (leaves, leaves), 0)
        cluster_c = lax.broadcasted_iota(jnp.int32, (leaves, leaves), 1)
        for level in range(local_levels):
            pick = (cluster_c >> level) == ((cluster_r >> level) ^ 1)
            partner = lax.dot_general(
                pick.astype(F32), fine, NN,
                precision=lax.Precision.HIGHEST, preferred_element_type=F32,
            )
            chosen = jnp.where(lane // rank == level, partner * scale_of(level), chosen)
        chosen = jnp.where(masks[0] > 0.0, chosen, 0.0)
        total = apply_far(None, chosen, 0, local_levels)
        wait_halo(step, halo_recv)
        extended = jnp.concatenate([halo[step, 0], own[step], halo[step, 1]], axis=0)
        leaf_no = lax.broadcasted_iota(jnp.int32, (3 * leaves, leaves), 0) + (me - 1) * leaves
        for k in range(nears):
            hot = jnp.broadcast_to(index[k:k + 1, :], (3 * leaves, leaves)) == leaf_no
            picks[k] = dot(hot.astype(F32).astype(BF16), extended, TN)

        def near_leaves(n, totals):
            totals = list(totals)
            for m in range(NEAR_UNROLL):
                i = n * NEAR_UNROLL + m
                for k in range(nears):
                    lhs = jnp.where(row == i, picks[k], 0.0).astype(BF16)
                    totals[m % 2] += dot(lhs, near[i, k], NT)
            return tuple(totals)

        totals = lax.fori_loop(
            0, leaves // NEAR_UNROLL, near_leaves, (total, jnp.zeros((leaves, leaf), F32))
        )
        partial[...] = totals[0] + totals[1]

    def apply_ring(pair, siblings):
        pair = pltpu.roll(spread(2, pair * scale_of(local_levels)), rank, 1)
        moved = pltpu.roll(spread(1, siblings * ring_scale), rank, 1)
        weights = jnp.concatenate([jnp.where(lane < rank, pair, moved), moved], axis=1)
        return apply_far(partial[...], weights, local_levels, local_levels + 1 + ring_bits)

    ring_scale = by_lane([scale_of(local_levels + 1 + j) for j in range(ring_bits)])
    plane_scale = by_lane([scale_of(levels - 2), scale_of(levels - 1)])
    ring_levels = (local_levels + 1, local_levels + 1 + ring_bits)

    def finish(step, total):
        out[step, pl.ds(0, leaves, 2), :] = total[:, :LANES]
        out[step, pl.ds(1, leaves, 2), :] = total[:, LANES:]

    def meet():
        pl.semaphore_wait(barrier, expected)
        for j in upper:
            @pl.when(bit(j) if j > quad_bits else outer)
            def _(j=j):
                pl.semaphore_signal(ready.at[j - quad_bits], inc=1, **target(peer_of(0, relay_step[j], 0)))

        for g in far_first[:-1]:
            pl.when(jnp.logical_not(plane_above(g)))(
                lambda g=g: pl.semaphore_signal(plane_ready.at[g], inc=1, **target(peer_of(g, 0, 0))))
        pl.when(jnp.logical_not(bottom))(
            lambda: pl.semaphore_signal(near_ready.at[0], inc=1, **target(left_of)))
        pl.when(top)(lambda: pl.semaphore_signal(near_ready.at[1], inc=1, **target(right_of)))

    last = spot == ring - 1
    late = spot >= ring - ring // 4
    pl.when(last)(meet)
    loads[0].wait()
    slip_rate = jnp.concatenate([slip[pl.ds(0, leaves, 2), :], slip[pl.ds(1, leaves, 2), :]], axis=1)
    vf = slip_rate.astype(BF16).astype(F32)
    last_local = write_mail(0, vf, pieces)
    pl.when(jnp.logical_not(last))(meet)
    def send_letter(t, sem):
        send(mail.at[0], got.at[t], level_send.at[sem], level_recv.at[sem], jnp.bitwise_xor(me, t))

    def send_down():
        for j, first_step, stride, length in runs:
            if j > quad_bits:
                def both(step):
                    for c in range(2):
                        send_letter(step * 2 + c, 0)
                run(first_step, stride, length, both)

    @pl.when(outer)
    def _():
        pl.when(jnp.logical_not(low))(send_down)
        for t in reversed(range(quad, 2 * quad)):
            send_letter(t, 2)

    for t in reversed(range(1, quad)):
        send_letter(t, 1)
    pl.when(jnp.logical_and(inner, jnp.logical_not(low)))(send_down)

    pl.when(jnp.logical_not(top))(lambda: pl.semaphore_wait(near_ready.at[0], 1))
    send_halo(0, 0)
    pl.when(jnp.logical_not(bottom))(lambda: send_halo(0, 1))

    def own_work():
        loads[2].wait()
        loads[3].wait()
        for group, held in enumerate((
            list(range(local_levels)), list(range(*ring_levels)),
            [levels - 2, levels - 1, None, local_levels],
        )):
            limit = jnp.zeros((leaves, LANES), jnp.int32)
            for part, level in enumerate(held):
                if level is not None:
                    column = jnp.broadcast_to(ranks[:, level:level + 1], (leaves, LANES))
                    limit = jnp.where(lane // rank == part, column, limit)
            masks[group] = (lane % rank < limit).astype(F32)
        for n in (4, 1, 5):
            loads[n].wait()
        local_part(0, vf, last_local)

    pl.when(late)(own_work)

    rows_done(got, quad - 1, level_recv.at[1])

    def sum_of(j, kind):
        return add_all(got[t, kind] for t in range(2 ** (j + 1), 2 ** (j + 2)))

    quad_ring = [sum_of(j, 0) for j in range(quad_bits)]
    known[0] = add_all([mail[0, 0], got[1, 0]] + quad_ring)
    known[1] = add_all([mail[0, 1], got[1, 1]] + [sum_of(j, 1) for j in range(quad_bits)])
    given = jnp.zeros((1, LANES), F32)
    for j in range(quad_bits):
        given = jnp.where(lane1 // rank == j, quad_ring[j], given)
    known[2] = given

    def take(j, ring_sum, far_sum):
        known[2] = jnp.where(lane1 // rank == j, ring_sum, known[2])
        known[0] = known[0] + ring_sum
        known[1] = known[1] + far_sum

    def settle_relay(n):
        part = got_relay.at[n]
        pltpu.make_async_copy(part, part, relay_recv.at[n]).wait()
        take(quad_bits + n, got_relay[n, 0], got_relay[n, 1])

    def send_relay(n):
        relay[n, 0] = known[0]
        relay[n, 1] = known[1]
        pl.semaphore_wait(ready.at[n], 1)
        send(relay.at[n], got_relay.at[n], relay_send.at[n], relay_recv.at[n],
             peer_of(0, relay_step[quad_bits + n], 0))

    pl.when(inner)(lambda: send_relay(0))

    @pl.when(bottom)
    def _():
        pl.semaphore_wait(near_ready.at[1], 1)
        send_halo(0, 1)

    def settle_half():
        pl.when(outer)(lambda: settle_relay(0))

        @pl.when(inner)
        def _():
            rows_done(got, quad, level_recv.at[2])
            take(quad_bits, sum_of(quad_bits, 0), sum_of(quad_bits, 1))

    @pl.when(low)
    def _():
        settle_half()
        send_relay(1)

    pl.when(jnp.logical_not(late))(own_work)
    @pl.when(jnp.logical_not(low))
    def _():
        settle_half()
        settle_relay(1)

    @pl.when(low)
    def _():
        rows_done(got, ring, level_recv.at[0])
        take(ring_bits - 1, sum_of(ring_bits - 1, 0), sum_of(ring_bits - 1, 1))

    plane_sums[...] = known[1]
    for g in far_first[:-1]:
        pl.when(plane_above(g))(lambda g=g: pl.semaphore_wait(plane_ready.at[g], 1))
        send(plane_sums, got_plane.at[g], plane_send.at[0], plane_recv.at[0], peer_of(g, 0, 0))
    total = apply_ring(got[1, 1], known[2])
    turn()
    rows_done(got_plane, groups - 1, plane_recv.at[0])
    far_sum = jnp.where(lane1 < rank, got_plane[1], add_all(got_plane[g] for g in range(2, groups)))
    first = apply_far(total, spread(2, far_sum * plane_scale), levels - FAR_BITS, levels)
    finish(0, first)

    relaxed = slip_rate + jnp.tanh(first / 3.0)
    vf = relaxed.astype(BF16).astype(F32)
    last_local = write_mail(1, vf)
    def send_row(g, step, c):
        sem = 1 if g else 0
        slot = g * plane + step * 2 + c
        send(mail.at[1, sem], got_all.at[slot], all_send.at[sem], all_recv.at[sem], peer_of(g, step, c))

    def all_of(step):
        for g in far_first:
            for c in range(2):
                send_row(g, step, c)

    for n, (_, first_step, stride, length) in enumerate(runs):
        run(first_step, stride, length, all_of)
        if n == 1:
            send_halo(1, 0)
            send_halo(1, 1)
    for g in far_first[:-1]:
        for c in range(2):
            send_row(g, 0, c)
    send(mail.at[1, 1], got_pair, pair_send.at[0], pair_recv.at[0], peer_of(0, 0, 1))
    local_part(1, vf, last_local)
    pltpu.make_async_copy(got_pair, got_pair, pair_recv.at[0]).wait()
    rows_done(got_all, plane - 2, all_recv.at[0])
    sibling = jnp.zeros((1, LANES), F32)
    for j in range(ring_bits):
        ring_sum = add_all(got_all[t] for t in range(2 ** (j + 1), 2 ** (j + 2)))
        sibling = jnp.where(lane1 // rank == j, ring_sum, sibling)
    total = apply_ring(got_pair[...], sibling)
    rows_done(got_all, count - plane, all_recv.at[1])
    far_sum = jnp.where(
        lane1 < rank, add_all(got_all[t] for t in range(plane, 2 * plane)),
        add_all(got_all[t] for t in range(2 * plane, count)),
    )
    finish(1, apply_far(total, spread(2, far_sum * plane_scale), levels - FAR_BITS, levels))

    for step in range(2):
        wait_halo(step, halo_send)
    rows_done(got, quad - 1, level_send.at[1])
    pl.when(inner)(
        lambda: pltpu.make_async_copy(relay.at[0], relay.at[0], relay_send.at[0]).wait())
    pl.when(outer)(lambda: rows_done(got, quad, level_send.at[2]))

    @pl.when(low)
    def _():
        pltpu.make_async_copy(relay.at[1], relay.at[1], relay_send.at[1]).wait()

    @pl.when(jnp.logical_not(low))
    def _():
        rows_done(got, ring, level_send.at[0])

    rows_done(got_plane, groups - 1, plane_send.at[0])
    rows_done(got_all, plane - 2, all_send.at[0])
    rows_done(got_all, count - plane, all_send.at[1])
    pltpu.make_async_copy(got_pair, got_pair, pair_send.at[0]).wait()


def write(out, first, second, sem):
    copies = [pltpu.make_async_copy(out.at[n], ref, sem.at[n]) for n, ref in enumerate((first, second))]
    for copy in copies:
        copy.start()
    for copy in copies:
        copy.wait()


def local(count, slip_rate, near_blocks, near_index, far_left, far_right, far_ranks):
    leaves, nears, leaf, _ = near_blocks.shape
    levels, rank, patches = far_left.shape
    cross = levels - (leaves.bit_length() - 1)
    ring_bits = cross - FAR_BITS - 1
    plane = count // 2**FAR_BITS
    assert (levels - leaves.bit_length() + 2) * rank == leaf
    assert leaf == 2 * LANES and 4 * rank == LANES and 2**cross == count
    assert leaves == 16 and ring_bits == 4
    flat = (patches // LANES, LANES)
    anywhere = pl.BlockSpec(memory_space=pl.ANY)
    dma = pltpu.SemaphoreType.DMA
    out = pl.pallas_call(
        functools.partial(kernel, (count, leaves, nears, leaf, levels, rank)),
        out_shape=pltpu.VMEM((2,) + flat, F32),
        in_specs=[anywhere] * 6,
        out_specs=pl.BlockSpec(memory_space=pltpu.VMEM),
        scratch_shapes=[
            pltpu.VMEM(flat, F32),
            pltpu.VMEM(far_ranks.shape, jnp.int32),
            pltpu.VMEM(near_index.shape[::-1], jnp.int32),
            pltpu.VMEM(far_right.shape, BF16),
            pltpu.VMEM(near_blocks.shape, BF16),
            pltpu.VMEM(far_left.shape, BF16),
            pltpu.VMEM((2, leaves, leaf), BF16),
            pltpu.VMEM((2, 2, leaves, leaf), BF16),
            pltpu.VMEM((3, leaves, LANES), F32),
            pltpu.VMEM((nears, leaves, leaf), F32),
            pltpu.VMEM((2, leaves, leaf), F32),
            pltpu.VMEM((leaves, leaf), F32),
            pltpu.VMEM((leaves, leaf, leaf), BF16),
            pltpu.VMEM((2, 2, 1, LANES), F32),
            pltpu.VMEM((plane, 2, 1, LANES), F32),
            pltpu.VMEM((3, 1, LANES), F32),
            pltpu.VMEM((2, 2, 1, LANES), F32),
            pltpu.VMEM((2, 2, 1, LANES), F32),
            pltpu.VMEM((1, LANES), F32),
            pltpu.VMEM((2**FAR_BITS, 1, LANES), F32),
            pltpu.VMEM((count, 1, LANES), F32),
            pltpu.VMEM((1, LANES), F32),
            dma((6,)), dma((PIECES,)), dma((2, 2)), dma((2, 2)),
            dma((3,)), dma((3,)), dma((2,)), dma((2,)),
            dma((1,)), dma((1,)), dma((2,)), dma((2,)), dma((1,)), dma((1,)),
            pltpu.SemaphoreType.REGULAR((2,)), pltpu.SemaphoreType.REGULAR((2,)),
            pltpu.SemaphoreType.REGULAR((2**FAR_BITS,)),
        ],
        compiler_params=pltpu.CompilerParams(collective_id=0, has_side_effects=True),
        name="hmatrix",
    )(slip_rate.reshape(flat), far_ranks, near_index.T, far_right, near_blocks, far_left)
    first, second = pl.pallas_call(
        write,
        out_shape=[jax.ShapeDtypeStruct(flat, F32)] * 2,
        in_specs=[pl.BlockSpec(memory_space=pltpu.VMEM)],
        out_specs=[anywhere] * 2,
        scratch_shapes=[dma((2,))],
        name="write",
    )(pltpu.with_memory_space_constraint(out, pltpu.VMEM))
    return first.reshape(-1), second.reshape(-1)


def solution(mesh):
    both = ("models", "leaf")
    in_specs = (
        P(both), P(both, None, None, None), P(both, None),
        P(None, None, both), P(None, None, both), P(both, None),
    )
    return jax.shard_map(
        functools.partial(local, mesh.shape["leaf"]), mesh=mesh, in_specs=in_specs,
        out_specs=(P(both), P(both)), check_vma=False,
    )
```

```python
import functools
import math

import jax
import jax.numpy as jnp
from jax import lax
from jax.experimental import pallas as pl
from jax.experimental.pallas import tpu as pltpu
from jax.sharding import PartitionSpec as P

MESH = pl.DeviceIdType.MESH
F32 = jnp.float32
BF16 = jnp.bfloat16
LANES = 128
FAR_BITS = 2
PIECES = 8
NEAR_UNROLL = 4
NT = (((1,), (1,)), ((), ()))
NN = (((1,), (0,)), ((), ()))
TN = (((0,), (0,)), ((), ()))


def dot(a, b, dims):
    return lax.dot_general(a, b, dims, preferred_element_type=F32)


def add_all(terms):
    terms = list(terms)
    while len(terms) > 1:
        odd = terms[len(terms) // 2 * 2:]
        terms = [x + y for x, y in zip(terms[::2], terms[1::2])] + odd
    return terms[0]


def kernel(
    shape,
    slip_hbm, ranks_hbm, index_hbm, right_hbm, near_hbm, left_hbm,
    out,
    slip, ranks, index, right, near, left, own, halo, masks, picks, sums, partial, turned,
    mail, got, known, relay, got_relay, plane_sums, got_plane, got_all, got_pair,
    load_sem, piece_sem, halo_send, halo_recv, level_send, level_recv, relay_send, relay_recv,
    plane_send, plane_recv, all_send, all_recv, pair_send, pair_recv, ready, near_ready, plane_ready,
):
    count, leaves, nears, leaf, levels, rank = shape
    local_levels = leaves.bit_length() - 1
    cross = levels - local_levels
    groups = 2**FAR_BITS
    plane = count // groups
    ring_bits = cross - FAR_BITS - 1
    ring = 2**ring_bits
    me = lax.axis_index("leaf")
    spot = lax.rem(me // 2, ring)

    def peer_of(far, step, core):
        return jnp.bitwise_xor(me, far * plane + step * 2 + core)

    def bit(j):
        return lax.rem(spot // 2**j, 2) == 1

    def target(peer):
        return dict(device_id={"leaf": peer}, device_id_type=MESH)

    right_of = lax.rem(me + 1, count)
    left_of = lax.rem(me + count - 1, count)
    far_first = [g for g in (2, 3, 1, 0) if g < groups]
    quad_bits = ring_bits - 2
    quad = 2 ** (quad_bits + 1)
    upper = range(quad_bits, ring_bits)
    relay_step = {quad_bits: ring // 4, quad_bits + 1: ring // 2 + ring // 4}
    half = ring // 2
    runs = [(ring_bits - 1, half, 1, half // 2), (ring_bits - 2, half - 1, -1, half // 2),
            (ring_bits - 1, half + half // 2, 1, half // 2)]
    runs += [(j, 2 ** (j + 1) - 1, -1, 2**j) for j in reversed(range(ring_bits - 2))]

    def run(first, stride, length, body):
        def trip(n, carry):
            body(first + stride * n)
            return carry

        lax.fori_loop(0, length, trip, 0)

    high = local_levels - 1
    piece = leaves // PIECES * leaf
    loads = [
        pltpu.make_async_copy(slip_hbm, slip, load_sem.at[0]),
        pltpu.make_async_copy(left_hbm, left, load_sem.at[1]),
        pltpu.make_async_copy(ranks_hbm, ranks, load_sem.at[2]),
        pltpu.make_async_copy(index_hbm, index, load_sem.at[3]),
        pltpu.make_async_copy(right_hbm.at[pl.ds(0, high)], right.at[pl.ds(0, high)], load_sem.at[4]),
        pltpu.make_async_copy(near_hbm, near, load_sem.at[5]),
    ]
    pieces = []
    for n in range(PIECES):
        part = (pl.ds(high, levels - high), slice(None), pl.ds(n * piece, piece))
        pieces.append(pltpu.make_async_copy(right_hbm.at[part], right.at[part], piece_sem.at[n]))
    loads[0].start()
    for load in pieces:
        load.start()

    barrier = pltpu.get_barrier_semaphore()

    def greet(peer):
        pl.semaphore_signal(barrier, inc=1, **target(peer))

    low = jnp.logical_not(bit(ring_bits - 1))
    outer = bit(ring_bits - 1) == bit(quad_bits)
    inner = jnp.logical_not(outer)
    plane_no = me // plane

    def plane_above(g):
        return lax.rem(plane_no // 2 ** (g.bit_length() - 1), 2) == 1

    for j, first_step, stride, length in runs:
        if j > quad_bits:
            @pl.when(low)
            def _(first_step=first_step, stride=stride, length=length):
                def both(step):
                    for c in range(2):
                        greet(peer_of(0, step, c))
                run(first_step, stride, length, both)
    expected = quad - 1
    for t in reversed(range(1, quad)):
        greet(peer_of(0, t // 2, t % 2))
    for g in far_first[:-1]:
        pl.when(plane_above(g))(lambda g=g: greet(peer_of(g, 0, 0)))
        expected = expected + jnp.where(plane_above(g), 0, 1)
    @pl.when(inner)
    def _():
        for t in reversed(range(quad, 2 * quad)):
            greet(peer_of(0, t // 2, t % 2))

    expected = expected + jnp.where(outer, quad, 0)
    expected = expected + jnp.where(low, 0, ring)
    top = jnp.logical_and(spot == ring - 1, lax.rem(me, 2) == 1)
    bottom = jnp.logical_and(spot == 0, lax.rem(me, 2) == 0)
    pl.when(jnp.logical_not(top))(lambda: greet(right_of))
    pl.when(bottom)(lambda: greet(left_of))
    expected = expected + jnp.where(bottom, 0, 1) + jnp.where(top, 1, 0)
    for load in (loads[2], loads[3], loads[4], loads[1], loads[5]):
        load.start()

    row = lax.broadcasted_iota(jnp.int32, (leaves, leaf), 0)
    row_l = lax.broadcasted_iota(jnp.int32, (leaves, LANES), 0)
    lane = lax.broadcasted_iota(jnp.int32, (leaves, LANES), 1)
    lane1 = lax.broadcasted_iota(jnp.int32, (1, LANES), 1)

    def scale_of(level):
        return 1.0 / math.sqrt(leaf * 2**level)

    def by_lane(values):
        scale = jnp.zeros((1, LANES), F32)
        for part, value in enumerate(values):
            scale = jnp.where(lane1 // rank == part, value, scale)
        return scale

    def turn():
        r = lax.broadcasted_iota(jnp.int32, (leaf, leaf), 0)
        eye = (r == lax.broadcasted_iota(jnp.int32, (leaf, leaf), 1)).astype(F32).astype(BF16)

        def pair_of(n, carry):
            for m in range(2):
                c = n * 2 + m
                block = right[high:levels, :, pl.ds(pl.multiple_of(c * leaf, leaf), leaf)]
                turned[c] = dot(eye, block.reshape(leaf, leaf), NT).astype(BF16)
            return carry

        lax.fori_loop(0, leaves // 2, pair_of, 0)

    def project_turned(vf):
        @pl.when(spot >= 0)
        def _():
            totals = [jnp.zeros((leaves, leaf), F32)] * 2
            for c in range(leaves):
                lhs = jnp.where(row == c, vf, 0.0).astype(BF16)
                totals[c % 2] += dot(lhs, turned[c], NN)
            for n in range(2):
                sums[n] = totals[n]

        return sums[0] + sums[1]

    def project(vf, start, stop, ready=()):
        rows = (stop - start) * rank
        @pl.when(spot >= 0)
        def _():
            totals = [jnp.zeros((leaves, rows), F32)] * 2
            for c in range(leaves):
                if ready and c % (leaves // PIECES) == 0:
                    ready[c // (leaves // PIECES)].wait()
                lhs = jnp.where(row == c, vf, 0.0).astype(BF16)
                rhs = right[start:stop, :, c * leaf:(c + 1) * leaf].reshape(rows, leaf)
                totals[c % 2] += dot(lhs, rhs, NT)
            for n in range(2):
                sums[n, :, :rows] = totals[n]

        return sums[0, :, :rows] + sums[1, :, :rows]

    def apply_far(total, weights, start, stop):
        rows = (stop - start) * rank
        row_w = lax.broadcasted_iota(jnp.int32, weights.shape, 0)

        @pl.when(spot >= 0)
        def _():
            totals = [jnp.zeros((leaves, leaf), F32)] * 2
            for i in range(leaves):
                lhs = jnp.where(row_w == i, weights, 0.0).astype(BF16)[:, :rows]
                rhs = left[start:stop, :, i * leaf:(i + 1) * leaf].reshape(rows, leaf)
                totals[i % 2] += dot(lhs, rhs, NN)
            for n in range(2):
                sums[n] = totals[n]

        return sums[0] + sums[1] if total is None else total + sums[0] + sums[1]

    def spread(mask, value):
        return jnp.where(masks[mask] > 0.0, jnp.broadcast_to(value, (leaves, LANES)), 0.0)

    def send(src, dst, send_sem, recv_sem, peer):
        pltpu.make_async_remote_copy(
            src_ref=src, dst_ref=dst, send_sem=send_sem, recv_sem=recv_sem, **target(peer)
        ).start()

    def rows_done(ref, rows, sem):
        part = ref.at[pl.ds(0, rows)]
        pltpu.make_async_copy(part, part, sem).wait()

    def write_mail(step, vf, ready=()):
        own[step] = vf.astype(BF16)
        summed = project_turned(vf) if step else project(vf, high, levels, ready)
        device_sums = jnp.sum(summed, axis=0, keepdims=True)
        one = pltpu.roll(device_sums[:, :LANES], 2 * rank, 1)
        two = pltpu.roll(device_sums[:, LANES:], 2 * rank, 1)
        mail[step, 0] = jnp.where(lane1 < 2 * rank, one, two)
        mail[step, 1] = jnp.where(lane1 < 2 * rank, two, one)
        return summed[:, :rank]

    def send_halo(step, side):
        send(own.at[step], halo.at[step, side], halo_send.at[step, side], halo_recv.at[step, side],
             left_of if side else right_of)

    def wait_halo(step, sems):
        for side in range(2):
            pltpu.make_async_copy(own.at[step], own.at[step], sems.at[step, side]).wait()

    def far_slot(g, step, c):
        return g * plane + step * 2 + c

    def local_part(step, vf, last_local):
        below = project(vf, 0, high)
        fine = jnp.concatenate([below, last_local], axis=1)
        chosen = jnp.zeros((leaves, LANES), F32)
        cluster_r = lax.broadcasted_iota(jnp.int32, (leaves, leaves), 0)
        cluster_c = lax.broadcasted_iota(jnp.int32, (leaves, leaves), 1)
        for level in range(local_levels):
            pick = (cluster_c >> level) == ((cluster_r >> level) ^ 1)
            partner = lax.dot_general(
                pick.astype(F32), fine, NN,
                precision=lax.Precision.HIGHEST, preferred_element_type=F32,
            )
            chosen = jnp.where(lane // rank == level, partner * scale_of(level), chosen)
        chosen = jnp.where(masks[0] > 0.0, chosen, 0.0)
        total = apply_far(None, chosen, 0, local_levels)
        wait_halo(step, halo_recv)
        extended = jnp.concatenate([halo[step, 0], own[step], halo[step, 1]], axis=0)
        leaf_no = lax.broadcasted_iota(jnp.int32, (3 * leaves, leaves), 0) + (me - 1) * leaves
        for k in range(nears):
            hot = jnp.broadcast_to(index[k:k + 1, :], (3 * leaves, leaves)) == leaf_no
            picks[k] = dot(hot.astype(F32).astype(BF16), extended, TN)

        def near_leaves(n, totals):
            totals = list(totals)
            for m in range(NEAR_UNROLL):
                i = n * NEAR_UNROLL + m
                for k in range(nears):
                    lhs = jnp.where(row == i, picks[k], 0.0).astype(BF16)
                    totals[m % 2] += dot(lhs, near[i, k], NT)
            return tuple(totals)

        totals = lax.fori_loop(
            0, leaves // NEAR_UNROLL, near_leaves, (total, jnp.zeros((leaves, leaf), F32))
        )
        partial[...] = totals[0] + totals[1]

    def apply_ring(pair, siblings):
        pair = pltpu.roll(spread(2, pair * scale_of(local_levels)), rank, 1)
        moved = pltpu.roll(spread(1, siblings * ring_scale), rank, 1)
        weights = jnp.concatenate([jnp.where(lane < rank, pair, moved), moved], axis=1)
        return apply_far(partial[...], weights, local_levels, local_levels + 1 + ring_bits)

    ring_scale = by_lane([scale_of(local_levels + 1 + j) for j in range(ring_bits)])
    plane_scale = by_lane([scale_of(levels - 2), scale_of(levels - 1)])
    ring_levels = (local_levels + 1, local_levels + 1 + ring_bits)

    def finish(step, total):
        out[step, pl.ds(0, leaves, 2), :] = total[:, :LANES]
        out[step, pl.ds(1, leaves, 2), :] = total[:, LANES:]

    def meet():
        pl.semaphore_wait(barrier, expected)
        for j in upper:
            @pl.when(bit(j) if j > quad_bits else outer)
            def _(j=j):
                pl.semaphore_signal(ready.at[j - quad_bits], inc=1, **target(peer_of(0, relay_step[j], 0)))

        for g in far_first[:-1]:
            pl.when(jnp.logical_not(plane_above(g)))(
                lambda g=g: pl.semaphore_signal(plane_ready.at[g], inc=1, **target(peer_of(g, 0, 0))))
        pl.when(jnp.logical_not(bottom))(
            lambda: pl.semaphore_signal(near_ready.at[0], inc=1, **target(left_of)))
        pl.when(top)(lambda: pl.semaphore_signal(near_ready.at[1], inc=1, **target(right_of)))

    last = spot == ring - 1
    late = spot >= ring - ring // 4
    pl.when(last)(meet)
    loads[0].wait()
    slip_rate = jnp.concatenate([slip[pl.ds(0, leaves, 2), :], slip[pl.ds(1, leaves, 2), :]], axis=1)
    vf = slip_rate.astype(BF16).astype(F32)
    last_local = write_mail(0, vf, pieces)
    pl.when(jnp.logical_not(last))(meet)
    def send_letter(t, sem):
        send(mail.at[0], got.at[t], level_send.at[sem], level_recv.at[sem], jnp.bitwise_xor(me, t))

    def send_down():
        for j, first_step, stride, length in runs:
            if j > quad_bits:
                def both(step):
                    for c in range(2):
                        send_letter(step * 2 + c, 0)
                run(first_step, stride, length, both)

    @pl.when(outer)
    def _():
        pl.when(jnp.logical_not(low))(send_down)
        for t in reversed(range(quad, 2 * quad)):
            send_letter(t, 2)

    for t in reversed(range(1, quad)):
        send_letter(t, 1)
    pl.when(jnp.logical_and(inner, jnp.logical_not(low)))(send_down)

    pl.when(jnp.logical_not(top))(lambda: pl.semaphore_wait(near_ready.at[0], 1))
    send_halo(0, 0)
    pl.when(jnp.logical_not(bottom))(lambda: send_halo(0, 1))

    def own_work():
        loads[2].wait()
        loads[3].wait()
        for group, held in enumerate((
            list(range(local_levels)), list(range(*ring_levels)),
            [levels - 2, levels - 1, None, local_levels],
        )):
            limit = jnp.zeros((leaves, LANES), jnp.int32)
            for part, level in enumerate(held):
                if level is not None:
                    column = jnp.broadcast_to(ranks[:, level:level + 1], (leaves, LANES))
                    limit = jnp.where(lane // rank == part, column, limit)
            masks[group] = (lane % rank < limit).astype(F32)
        for n in (4, 1, 5):
            loads[n].wait()
        local_part(0, vf, last_local)

    pl.when(late)(own_work)

    rows_done(got, quad - 1, level_recv.at[1])

    def sum_of(j, kind):
        return add_all(got[t, kind] for t in range(2 ** (j + 1), 2 ** (j + 2)))

    quad_ring = [sum_of(j, 0) for j in range(quad_bits)]
    known[0] = add_all([mail[0, 0], got[1, 0]] + quad_ring)
    known[1] = add_all([mail[0, 1], got[1, 1]] + [sum_of(j, 1) for j in range(quad_bits)])
    given = jnp.zeros((1, LANES), F32)
    for j in range(quad_bits):
        given = jnp.where(lane1 // rank == j, quad_ring[j], given)
    known[2] = given

    def take(j, ring_sum, far_sum):
        known[2] = jnp.where(lane1 // rank == j, ring_sum, known[2])
        known[0] = known[0] + ring_sum
        known[1] = known[1] + far_sum

    def settle_relay(n):
        part = got_relay.at[n]
        pltpu.make_async_copy(part, part, relay_recv.at[n]).wait()
        take(quad_bits + n, got_relay[n, 0], got_relay[n, 1])

    def send_relay(n):
        relay[n, 0] = known[0]
        relay[n, 1] = known[1]
        pl.semaphore_wait(ready.at[n], 1)
        send(relay.at[n], got_relay.at[n], relay_send.at[n], relay_recv.at[n],
             peer_of(0, relay_step[quad_bits + n], 0))

    pl.when(inner)(lambda: send_relay(0))

    @pl.when(bottom)
    def _():
        pl.semaphore_wait(near_ready.at[1], 1)
        send_halo(0, 1)

    def settle_half():
        pl.when(outer)(lambda: settle_relay(0))

        @pl.when(inner)
        def _():
            rows_done(got, quad, level_recv.at[2])
            take(quad_bits, sum_of(quad_bits, 0), sum_of(quad_bits, 1))

    @pl.when(low)
    def _():
        settle_half()
        send_relay(1)

    pl.when(jnp.logical_not(late))(own_work)
    @pl.when(jnp.logical_not(low))
    def _():
        settle_half()
        settle_relay(1)

    @pl.when(low)
    def _():
        rows_done(got, ring, level_recv.at[0])
        take(ring_bits - 1, sum_of(ring_bits - 1, 0), sum_of(ring_bits - 1, 1))

    plane_sums[...] = known[1]
    for g in far_first[:-1]:
        pl.when(plane_above(g))(lambda g=g: pl.semaphore_wait(plane_ready.at[g], 1))
        send(plane_sums, got_plane.at[g], plane_send.at[0], plane_recv.at[0], peer_of(g, 0, 0))
    total = apply_ring(got[1, 1], known[2])
    turn()
    rows_done(got_plane, groups - 1, plane_recv.at[0])
    far_sum = jnp.where(lane1 < rank, got_plane[1], add_all(got_plane[g] for g in range(2, groups)))
    first = apply_far(total, spread(2, far_sum * plane_scale), levels - FAR_BITS, levels)
    finish(0, first)

    relaxed = slip_rate + jnp.tanh(first / 3.0)
    vf = relaxed.astype(BF16).astype(F32)
    last_local = write_mail(1, vf)
    def send_row(g, step, c):
        sem = 1 if g else 0
        slot = g * plane + step * 2 + c
        send(mail.at[1, sem], got_all.at[slot], all_send.at[sem], all_recv.at[sem], peer_of(g, step, c))

    def all_of(step):
        for g in far_first:
            for c in range(2):
                send_row(g, step, c)

    for n, (_, first_step, stride, length) in enumerate(runs):
        run(first_step, stride, length, all_of)
        if n == 1:
            send_halo(1, 0)
            send_halo(1, 1)
    for g in far_first[:-1]:
        for c in range(2):
            send_row(g, 0, c)
    send(mail.at[1, 1], got_pair, pair_send.at[0], pair_recv.at[0], peer_of(0, 0, 1))
    local_part(1, vf, last_local)
    pltpu.make_async_copy(got_pair, got_pair, pair_recv.at[0]).wait()
    rows_done(got_all, plane - 2, all_recv.at[0])
    sibling = jnp.zeros((1, LANES), F32)
    for j in range(ring_bits):
        ring_sum = add_all(got_all[t] for t in range(2 ** (j + 1), 2 ** (j + 2)))
        sibling = jnp.where(lane1 // rank == j, ring_sum, sibling)
    total = apply_ring(got_pair[...], sibling)
    rows_done(got_all, count - plane, all_recv.at[1])
    far_sum = jnp.where(
        lane1 < rank, add_all(got_all[t] for t in range(plane, 2 * plane)),
        add_all(got_all[t] for t in range(2 * plane, count)),
    )
    finish(1, apply_far(total, spread(2, far_sum * plane_scale), levels - FAR_BITS, levels))

    for step in range(2):
        wait_halo(step, halo_send)
    rows_done(got, quad - 1, level_send.at[1])
    pl.when(inner)(
        lambda: pltpu.make_async_copy(relay.at[0], relay.at[0], relay_send.at[0]).wait())
    pl.when(outer)(lambda: rows_done(got, quad, level_send.at[2]))

    @pl.when(low)
    def _():
        pltpu.make_async_copy(relay.at[1], relay.at[1], relay_send.at[1]).wait()

    @pl.when(jnp.logical_not(low))
    def _():
        rows_done(got, ring, level_send.at[0])

    rows_done(got_plane, groups - 1, plane_send.at[0])
    rows_done(got_all, plane - 2, all_send.at[0])
    rows_done(got_all, count - plane, all_send.at[1])
    pltpu.make_async_copy(got_pair, got_pair, pair_send.at[0]).wait()


def write(out, first, second, sem):
    copies = [pltpu.make_async_copy(out.at[n], ref, sem.at[n]) for n, ref in enumerate((first, second))]
    for copy in copies:
        copy.start()
    for copy in copies:
        copy.wait()


def local(count, slip_rate, near_blocks, near_index, far_left, far_right, far_ranks):
    leaves, nears, leaf, _ = near_blocks.shape
    levels, rank, patches = far_left.shape
    cross = levels - (leaves.bit_length() - 1)
    ring_bits = cross - FAR_BITS - 1
    plane = count // 2**FAR_BITS
    assert (levels - leaves.bit_length() + 2) * rank == leaf
    assert leaf == 2 * LANES and 4 * rank == LANES and 2**cross == count
    assert leaves == 16 and ring_bits == 4
    flat = (patches // LANES, LANES)
    anywhere = pl.BlockSpec(memory_space=pl.ANY)
    dma = pltpu.SemaphoreType.DMA
    out = pl.pallas_call(
        functools.partial(kernel, (count, leaves, nears, leaf, levels, rank)),
        out_shape=pltpu.VMEM((2,) + flat, F32),
        in_specs=[anywhere] * 6,
        out_specs=pl.BlockSpec(memory_space=pltpu.VMEM),
        scratch_shapes=[
            pltpu.VMEM(flat, F32),
            pltpu.VMEM(far_ranks.shape, jnp.int32),
            pltpu.VMEM(near_index.shape[::-1], jnp.int32),
            pltpu.VMEM(far_right.shape, BF16),
            pltpu.VMEM(near_blocks.shape, BF16),
            pltpu.VMEM(far_left.shape, BF16),
            pltpu.VMEM((2, leaves, leaf), BF16),
            pltpu.VMEM((2, 2, leaves, leaf), BF16),
            pltpu.VMEM((3, leaves, LANES), F32),
            pltpu.VMEM((nears, leaves, leaf), F32),
            pltpu.VMEM((2, leaves, leaf), F32),
            pltpu.VMEM((leaves, leaf), F32),
            pltpu.VMEM((leaves, leaf, leaf), BF16),
            pltpu.VMEM((2, 2, 1, LANES), F32),
            pltpu.VMEM((plane, 2, 1, LANES), F32),
            pltpu.VMEM((3, 1, LANES), F32),
            pltpu.VMEM((2, 2, 1, LANES), F32),
            pltpu.VMEM((2, 2, 1, LANES), F32),
            pltpu.VMEM((1, LANES), F32),
            pltpu.VMEM((2**FAR_BITS, 1, LANES), F32),
            pltpu.VMEM((count, 1, LANES), F32),
            pltpu.VMEM((1, LANES), F32),
            dma((6,)), dma((PIECES,)), dma((2, 2)), dma((2, 2)),
            dma((3,)), dma((3,)), dma((2,)), dma((2,)),
            dma((1,)), dma((1,)), dma((2,)), dma((2,)), dma((1,)), dma((1,)),
            pltpu.SemaphoreType.REGULAR((2,)), pltpu.SemaphoreType.REGULAR((2,)),
            pltpu.SemaphoreType.REGULAR((2**FAR_BITS,)),
        ],
        compiler_params=pltpu.CompilerParams(collective_id=0, has_side_effects=True),
        name="hmatrix",
    )(slip_rate.reshape(flat), far_ranks, near_index.T, far_right, near_blocks, far_left)
    first, second = pl.pallas_call(
        write,
        out_shape=[jax.ShapeDtypeStruct(flat, F32)] * 2,
        in_specs=[pl.BlockSpec(memory_space=pltpu.VMEM)],
        out_specs=[anywhere] * 2,
        scratch_shapes=[dma((2,))],
        name="write",
    )(pltpu.with_memory_space_constraint(out, pltpu.VMEM))
    return first.reshape(-1), second.reshape(-1)


def solution(mesh):
    both = ("models", "leaf")
    in_specs = (
        P(both), P(both, None, None, None), P(both, None),
        P(None, None, both), P(None, None, both), P(both, None),
    )
    return jax.shard_map(
        functools.partial(local, mesh.shape["leaf"]), mesh=mesh, in_specs=in_specs,
        out_specs=(P(both), P(both)), check_vma=False,
    )
```
